32 devices in a mesh: py: 4 (over y, x), pz: 8 (over z, core).
Axes of the slice: x: 2, y: 2, z: 4, core: 2. Of those that a mesh axis runs over, the one named last changes fastest.
Arguments:
- species: float32 [4, 512, 64, 64], P(None, None, 'py', 'pz'), may hold values from -6 to 6
- coupling: float32 [4, 4], replicated, may hold values from -4 to 4
- symbol_x: float32 [512], replicated, may hold values from 0.3 to 3
- symbol_y: float32 [64], replicated, may hold values from 0.3 to 3
- symbol_z: float32 [64], replicated, may hold values from 0.3 to 3
Outputs:
- modes: float32 [4, 512, 64, 64], P(None, 'py', 'pz')
The draws below stay inside these ranges and needn't reach their ends.
All inputs are finite; a program needn't handle non-finite values.
Results may differ from the reference program's by a relative error of at most 0.00007.
Values sent between devices are 32-bit elements; how exact they have to be, the bound alone decides.
A program may use at most 64 MiB of HBM per device.

```python
import jax
import jax.numpy as jnp
from jax import lax

GRID_X = 512
GRID_Y = 64
GRID_Z = 64
FIELDS = 4


def block_levels(key, shape, pieces, low, largest):
    def one(dim, shards_of):
        draws = jax.random.uniform(jax.random.fold_in(jax.random.fold_in(key, 6), dim), (shards_of,), jnp.float32, low / len(pieces), largest / len(pieces))
        return jnp.repeat(jnp.exp(draws), shape[dim] // shards_of).reshape((-1,) + (1,) * (len(shape) - dim - 1))

    gain = one(*pieces[0])
    for cut in pieces[1:]:
        gain = gain * one(*cut)
    return gain


def bell_draw(rng, shape, spread, most, shards=(), dtype=jnp.bfloat16):
    result = spread * jax.random.normal(rng, shape, jnp.float32)
    if shards:
        result = result * block_levels(rng, shape, shards, -0.22, 0.18)
    return jnp.clip(result, -most, most).astype(dtype)


def setup_inputs(seed: int = 0) -> dict:
    key_list = jax.random.split(jax.random.key(seed), 6)
    return {
        "species": bell_draw(key_list[0], (FIELDS, GRID_X, GRID_Y, GRID_Z), 1.0, 6.0, ((2, 4), (3, 8)), jnp.float32),
        "coupling": bell_draw(key_list[1], (FIELDS, FIELDS), 0.7, 4.0, (), jnp.float32),
        "symbol_x": jnp.clip(jax.random.uniform(key_list[2], (GRID_X,), jnp.float32, 0.3, 3.0), 0.3, 3.0),
        "symbol_y": jnp.clip(jax.random.uniform(key_list[3], (GRID_Y,), jnp.float32, 0.3, 3.0), 0.3, 3.0),
        "symbol_z": jnp.clip(jax.random.uniform(key_list[4], (GRID_Z,), jnp.float32, 0.3, 3.0), 0.3, 3.0),
    }


def mode_table(count):
    rank = jnp.arange(count)
    angle = (jnp.pi / (4 * count)) * (((2 * rank[:, None] + 1) * (2 * rank[None, :] + 1)) % (8 * count)).astype(jnp.float32)
    return jnp.cos(angle) * (2.0 / count) ** 0.5


def transform_dim(values, dim):
    moved = jnp.tensordot(values, mode_table(values.shape[dim]), axes=([dim], [0]), precision=lax.Precision.HIGHEST)
    return jnp.moveaxis(moved, -1, dim)


def reference(species, coupling, symbol_x, symbol_y, symbol_z):
    modes = species
    modes = transform_dim(modes, 1)
    modes = transform_dim(modes, 2)
    modes = transform_dim(modes, 3)
    symbol = symbol_x[:, None, None] + symbol_y[None, :, None] + symbol_z[None, None, :]
    weight_xyz = 1.0 / (1.0 + symbol)
    mixed_fields = jnp.einsum("ab,bxyz->axyz", coupling, modes, precision=lax.Precision.HIGHEST)
    modes = weight_xyz * modes + (1.0 - weight_xyz) * mixed_fields
    return modes
```

```python
import functools

import jax
import jax.numpy as jnp
import numpy as np
from jax import lax
from jax.experimental import pallas as pl
from jax.experimental.pallas import tpu as pltpu
from jax.sharding import PartitionSpec as P

MESH = pl.DeviceIdType.MESH
F32 = jnp.float32
BF16 = jnp.bfloat16
LANES, SUBLANES = 128, 8
VMEM_BUDGET = 48 << 20


def mode_table(count):
    rank = jnp.arange(count)
    angle = (
        jnp.pi
        / (4 * count)
        * ((2 * rank[:, None] + 1) * (2 * rank[None, :] + 1) % (8 * count)).astype(jnp.float32)
    )
    return jnp.cos(angle) * (2.0 / count) ** 0.5


def transform_dim(values, dim):
    moved = jnp.tensordot(
        values, mode_table(values.shape[dim]), axes=([dim], [0]), precision=lax.Precision.HIGHEST
    )
    return jnp.moveaxis(moved, -1, dim)


def plain_shards(species, coupling, symbol_x, symbol_y, symbol_z):
    values = transform_dim(species, 1)
    values = lax.all_to_all(values, "py", split_axis=1, concat_axis=2, tiled=True)
    values = transform_dim(values, 2)
    values = lax.all_to_all(values, "pz", split_axis=2, concat_axis=3, tiled=True)
    values = transform_dim(values, 3)
    share_x = values.shape[1]
    part_x = lax.dynamic_slice_in_dim(symbol_x, lax.axis_index("py") * share_x, share_x)
    share_y = values.shape[2]
    part_y = lax.dynamic_slice_in_dim(symbol_y, lax.axis_index("pz") * share_y, share_y)
    symbol = part_x[:, None, None] + part_y[None, :, None] + symbol_z[None, None, :]
    weight = 1.0 / (1.0 + symbol)
    mixed = jnp.einsum("ab,bxyz->axyz", coupling, values, precision=lax.Precision.HIGHEST)
    return weight * values + (1.0 - weight) * mixed


def split_table(count):
    rank = 2 * np.arange(count) + 1
    table = np.cos(np.pi / (4 * count) * (rank[:, None] * rank[None, :] % (8 * count)))
    table = (table * np.sqrt(2.0 / count)).astype(np.float32)
    high = table.astype(BF16)
    low = (table - high.astype(np.float32)).astype(BF16)
    return np.stack([high, low])


def split(values):
    high = values.astype(BF16)
    low = (values - high.astype(F32)).astype(BF16)
    return high, low


def dot(a, b):
    return jnp.dot(a, b, preferred_element_type=F32)


def flipped(index, offset, count):
    if count & (count - 1):
        return lax.rem(index + offset, count)
    result = index
    bit = 1
    while bit < count:
        if offset & bit:
            result = result + bit - 2 * bit * lax.rem(index // bit, 2)
        bit *= 2
    return result


def source_of(index, offset, count):
    if count & (count - 1):
        return lax.rem(index + count - offset, count)
    return flipped(index, offset, count)


def kernel(
    dims, field_ref, hx_hbm, hy_hbm, hz_hbm, coupling_hbm, sx_hbm, sy_hbm, sz_hbm, out_ref,
    held, hx, hy, hz, coupling, sx, sy, sz, lines_out, lines, parts_out, parts, modes, weights,
    my, mz, load_sem, side_sem, send_y, recv_y, send_z, recv_z,
):
    fields, ny, nz, n_py, n_pz, yl, zl, share_x, share_y = dims
    py, pz = lax.axis_index("py"), lax.axis_index("pz")
    rows_y = yl * zl
    rows_z = share_y * zl
    depth_y = ny * zl
    rows_out = share_y * nz
    depth_z = n_pz * rows_z

    def load(f):
        return pltpu.make_async_copy(field_ref.at[f], held.at[f], load_sem.at[f])

    pairs = (
        (hx_hbm.at[0], hx.at[0]), (hx_hbm.at[1], hx.at[1]), (hy_hbm, hy), (hz_hbm, hz),
        (coupling_hbm, coupling), (sx_hbm, sx), (sy_hbm, sy), (sz_hbm, sz),
    )
    sides = [
        pltpu.make_async_copy(a, b, side_sem.at[i]) for i, (a, b) in enumerate(pairs)
    ]
    load(0).start()
    sides[0].start()
    sides[1].start()
    for f in range(1, fields):
        load(f).start()
    for side in sides[2:]:
        side.start()
    barrier = pltpu.get_barrier_semaphore()
    for o in range(1, n_pz):
        pl.semaphore_signal(
            barrier, inc=1, device_id={"pz": flipped(pz, o, n_pz)}, device_id_type=MESH
        )
    for o in range(1, n_py):
        pl.semaphore_signal(
            barrier, inc=1, device_id={"py": flipped(py, o, n_py)}, device_id_type=MESH
        )

    def copy_y(f, o):
        to = flipped(py, o, n_py)
        return pltpu.make_async_remote_copy(
            src_ref=lines_out.at[f, to],
            dst_ref=lines.at[f, pl.ds(py * rows_y, rows_y)],
            send_sem=send_y.at[f, o],
            recv_sem=recv_y.at[f, o],
            device_id={"py": to},
            device_id_type=MESH,
        )

    def copy_z(f, o):
        to = flipped(pz, o, n_pz)
        return pltpu.make_async_remote_copy(
            src_ref=parts_out.at[f, pl.ds(to * rows_z, rows_z)],
            dst_ref=parts.at[f, pl.ds(pz * rows_z, rows_z)],
            send_sem=send_z.at[f, o],
            recv_sem=recv_z.at[f, o],
            device_id={"pz": to},
            device_id_type=MESH,
        )

    for f in range(fields):
        load(f).wait()
        high, low = split(held[f])
        if f == 0:
            sides[0].wait()
            sides[1].wait()
        both = dot(jnp.concatenate([high, low], axis=0), hx[0])
        result = both[:rows_y] + both[rows_y:] + dot(high, hx[1])
        for d in range(n_py):
            lines_out[f, d] = result[:, d * share_x : (d + 1) * share_x]
        if f == 0:
            pl.semaphore_wait(barrier, n_py + n_pz - 2)
        for o in range(n_py - 1, 0, -1):
            copy_y(f, o).start()
        lines[f, pl.ds(py * rows_y, rows_y)] = lines_out[f, py]

    for side in sides[2:]:
        side.wait()

    def iota(shape, dim):
        return lax.broadcasted_iota(jnp.int32, shape, dim)

    row, col = iota((depth_y, ny), 0), iota((depth_y, ny), 1)
    pick = (row // zl == col).astype(F32).astype(BF16)
    row, col = iota((ny, depth_y), 0), iota((ny, depth_y), 1)
    spread = (col // zl == row).astype(F32).astype(BF16)
    row, col = iota((depth_y, depth_y), 0), iota((depth_y, depth_y), 1)
    keep = row % zl == col % zl
    for t in range(2):
        wide = dot(dot(pick, hy[t]).astype(BF16), spread)
        my[t] = jnp.where(keep, wide, 0.0).astype(BF16)
    def rows_transform(high_table, low_table, high, low):
        both = dot(high_table, jnp.concatenate([high, low], axis=1))
        return both[:, :share_x] + both[:, share_x:] + dot(low_table, high)

    halves = 2 if n_pz % 2 == 0 and n_pz & (n_pz - 1) == 0 else 1
    half_rows = depth_y // halves
    for f in range(fields):
        for o in range(n_py - 1, 0, -1):
            copy_y(f, o).wait_recv()
        high, low = split(lines[f])
        for h in range(halves):
            part = lax.rem(pz // (n_pz // halves) + h + 1, halves)
            span = pl.ds(pl.multiple_of(part * half_rows, half_rows), half_rows)
            parts_out[f, span] = rows_transform(my[0, span], my[1, span], high, low)
            top = n_pz - h * (n_pz // halves)
            for o in range(top - 1, max(top - n_pz // halves, 1) - 1, -1):
                copy_z(f, o).start()
        parts[f, pl.ds(pz * rows_z, rows_z)] = parts_out[f, pl.ds(pz * rows_z, rows_z)]

    row, col = iota((rows_out, nz), 0), iota((rows_out, nz), 1)
    pick = (row % nz == col).astype(F32).astype(BF16)
    row, col = iota((nz, depth_z), 0), iota((nz, depth_z), 1)
    spread = ((col // rows_z) * zl + col % zl == row).astype(F32).astype(BF16)
    row, col = iota((rows_out, depth_z), 0), iota((rows_out, depth_z), 1)
    keep = row // nz == (col // zl) % share_y
    for t in range(2):
        wide = dot(dot(pick, hz[t]).astype(BF16), spread)
        mz[t] = jnp.where(keep, wide, 0.0).astype(BF16)

    diagonal = iota((nz, nz), 0) == iota((nz, nz), 1)
    sz_column = jnp.sum(jnp.where(diagonal, sz[...], 0.0), axis=1, keepdims=True)
    sx_row = sx[:, pl.ds(pl.multiple_of(py * share_x, share_x), share_x)]
    for k in range(share_y):
        symbol = (sx_row + sy[pz * share_y + k]) + sz_column
        weights[pl.ds(k * nz, nz)] = 1.0 / (1.0 + symbol)

    last = fields - 1
    for f in range(fields):
        for o in range(n_pz - 1, 0, -1):
            copy_z(f, o).wait_recv()
        high, low = split(parts[f])
        if f < last:
            modes[f] = rows_transform(mz[0], mz[1], high, low)
        if f == last - 1:
            for k in range(share_y):
                span = pl.ds(k * nz, nz)
                weight = weights[span]
                old = [modes[b, span] for b in range(last)]
                for a in range(fields):
                    mixed = coupling[a, 0] * old[0]
                    for b in range(1, last):
                        mixed = mixed + coupling[a, b] * old[b]
                    mixed = (1.0 - weight) * mixed
                    out_ref[a, span] = mixed + weight * old[a] if a < last else mixed
        if f == last:
            result = rows_transform(mz[0], mz[1], high, low)
            weight = weights[...]
            rest = (1.0 - weight) * result
            for a in range(fields):
                new = out_ref[a] + coupling[a, last] * rest
                out_ref[a] = new + weight * result if a == last else new
    for f in range(fields):
        for o in range(1, n_py):
            copy_y(f, o).wait_send()
        for o in range(1, n_pz):
            copy_z(f, o).wait_send()


def shards(n_py, n_pz, species, coupling, symbol_x, symbol_y, symbol_z):
    fields, nx, yl, zl = species.shape
    ny, nz = yl * n_py, zl * n_pz
    share_x, share_y = nx // n_py, ny // n_pz
    block = fields * nx * yl * zl
    tables = 2 * (nx * nx + (ny * zl) ** 2 + (share_y * nz) ** 2)
    need = 7 * 4 * block + 2 * tables + 16 * max(ny * zl, share_y * nz) ** 2
    if share_x % LANES or zl % SUBLANES or nx % n_py or ny % n_pz or need > VMEM_BUDGET or fields < 2:
        return plain_shards(species, coupling, symbol_x, symbol_y, symbol_z)
    dims = (fields, ny, nz, n_py, n_pz, yl, zl, share_x, share_y)
    rows_y, depth_y, depth_z = yl * zl, ny * zl, share_y * nz
    vmem = pl.BlockSpec(memory_space=pltpu.VMEM)
    hbm = pl.BlockSpec(memory_space=pltpu.HBM)
    values = jnp.transpose(species, (0, 2, 3, 1)).reshape(fields, rows_y, nx)
    out = pl.pallas_call(
        functools.partial(kernel, dims),
        out_shape=jax.ShapeDtypeStruct((fields, depth_z, share_x), F32),
        in_specs=[hbm] * 8,
        out_specs=vmem,
        scratch_shapes=[
            pltpu.VMEM((fields, rows_y, nx), F32),
            pltpu.VMEM((2, nx, nx), BF16),
            pltpu.VMEM((2, ny, ny), BF16),
            pltpu.VMEM((2, nz, nz), BF16),
            pltpu.SMEM((fields, fields), F32),
            pltpu.VMEM((1, nx), F32),
            pltpu.SMEM((ny,), F32),
            pltpu.VMEM((1, nz), F32),
            pltpu.VMEM((fields, n_py, rows_y, share_x), F32),
            pltpu.VMEM((fields, depth_y, share_x), F32),
            pltpu.VMEM((fields, depth_y, share_x), F32),
            pltpu.VMEM((fields, depth_z, share_x), F32),
            pltpu.VMEM((fields - 1, depth_z, share_x), F32),
            pltpu.VMEM((depth_z, share_x), F32),
            pltpu.VMEM((2, depth_y, depth_y), BF16),
            pltpu.VMEM((2, depth_z, depth_z), BF16),
            pltpu.SemaphoreType.DMA((fields,)),
            pltpu.SemaphoreType.DMA((8,)),
            pltpu.SemaphoreType.DMA((fields, n_py)),
            pltpu.SemaphoreType.DMA((fields, n_py)),
            pltpu.SemaphoreType.DMA((fields, n_pz)),
            pltpu.SemaphoreType.DMA((fields, n_pz)),
        ],
        compiler_params=pltpu.CompilerParams(
            collective_id=0, has_side_effects=True, vmem_limit_bytes=54500000
        ),
    )(
        *(
            pltpu.with_memory_space_constraint(x, pltpu.HBM)
            for x in (
                values,
                jnp.asarray(split_table(nx)),
                jnp.asarray(split_table(ny)),
                jnp.asarray(split_table(nz)),
                coupling,
                symbol_x.reshape(1, nx),
                symbol_y,
                symbol_z.reshape(1, nz),
            )
        )
    )
    return jnp.transpose(out.reshape(fields, share_y, nz, share_x), (0, 3, 1, 2))


def solution(mesh):
    return jax.shard_map(
        functools.partial(shards, mesh.shape["py"], mesh.shape["pz"]),
        mesh=mesh,
        in_specs=(P(None, None, "py", "pz"), P(), P(), P(), P()),
        out_specs=P(None, "py", "pz", None),
        check_vma=False,
    )
```

```python
import functools

import jax
import jax.numpy as jnp
import numpy as np
from jax import lax
from jax.experimental import pallas as pl
from jax.experimental.pallas import tpu as pltpu
from jax.sharding import PartitionSpec as P

MESH = pl.DeviceIdType.MESH
F32 = jnp.float32
BF16 = jnp.bfloat16
LANES, SUBLANES = 128, 8
VMEM_BUDGET = 48 << 20


def mode_table(count):
    rank = jnp.arange(count)
    angle = (
        jnp.pi
        / (4 * count)
        * ((2 * rank[:, None] + 1) * (2 * rank[None, :] + 1) % (8 * count)).astype(jnp.float32)
    )
    return jnp.cos(angle) * (2.0 / count) ** 0.5


def transform_dim(values, dim):
    moved = jnp.tensordot(
        values, mode_table(values.shape[dim]), axes=([dim], [0]), precision=lax.Precision.HIGHEST
    )
    return jnp.moveaxis(moved, -1, dim)


def plain_shards(species, coupling, symbol_x, symbol_y, symbol_z):
    values = transform_dim(species, 1)
    values = lax.all_to_all(values, "py", split_axis=1, concat_axis=2, tiled=True)
    values = transform_dim(values, 2)
    values = lax.all_to_all(values, "pz", split_axis=2, concat_axis=3, tiled=True)
    values = transform_dim(values, 3)
    share_x = values.shape[1]
    part_x = lax.dynamic_slice_in_dim(symbol_x, lax.axis_index("py") * share_x, share_x)
    share_y = values.shape[2]
    part_y = lax.dynamic_slice_in_dim(symbol_y, lax.axis_index("pz") * share_y, share_y)
    symbol = part_x[:, None, None] + part_y[None, :, None] + symbol_z[None, None, :]
    weight = 1.0 / (1.0 + symbol)
    mixed = jnp.einsum("ab,bxyz->axyz", coupling, values, precision=lax.Precision.HIGHEST)
    return weight * values + (1.0 - weight) * mixed


def split_table(count):
    rank = 2 * np.arange(count) + 1
    table = np.cos(np.pi / (4 * count) * (rank[:, None] * rank[None, :] % (8 * count)))
    table = (table * np.sqrt(2.0 / count)).astype(np.float32)
    high = table.astype(BF16)
    low = (table - high.astype(np.float32)).astype(BF16)
    return np.stack([high, low])


def split(values):
    high = values.astype(BF16)
    low = (values - high.astype(F32)).astype(BF16)
    return high, low


def dot(a, b):
    return jnp.dot(a, b, preferred_element_type=F32)


def flipped(index, offset, count):
    if count & (count - 1):
        return lax.rem(index + offset, count)
    result = index
    bit = 1
    while bit < count:
        if offset & bit:
            result = result + bit - 2 * bit * lax.rem(index // bit, 2)
        bit *= 2
    return result


def source_of(index, offset, count):
    if count & (count - 1):
        return lax.rem(index + count - offset, count)
    return flipped(index, offset, count)


def kernel(
    dims, field_ref, hx_hbm, hy_hbm, hz_hbm, coupling_hbm, sx_hbm, sy_hbm, sz_hbm, out_ref,
    held, hx, hy, hz, coupling, sx, sy, sz, lines_out, lines, parts_out, parts, modes, weights,
    my, mz, far, far_lines, far_out, load_sem, side_sem, send_y, recv_y, send_z, recv_z,
    send_raw, recv_raw, send_relay, recv_relay, send_far, recv_far,
):
    fields, ny, nz, n_py, n_pz, yl, zl, share_x, share_y = dims
    py, pz = lax.axis_index("py"), lax.axis_index("pz")
    rows_y = yl * zl
    rows_z = share_y * zl
    depth_y = ny * zl
    rows_out = share_y * nz
    depth_z = n_pz * rows_z

    def load(f):
        return pltpu.make_async_copy(field_ref.at[f], held.at[f], load_sem.at[f])

    pairs = (
        (hx_hbm.at[0], hx.at[0]), (hx_hbm.at[1], hx.at[1]), (hy_hbm, hy), (hz_hbm, hz),
        (coupling_hbm, coupling), (sx_hbm, sx), (sy_hbm, sy), (sz_hbm, sz),
    )
    sides = [
        pltpu.make_async_copy(a, b, side_sem.at[i]) for i, (a, b) in enumerate(pairs)
    ]
    barrier = pltpu.get_barrier_semaphore()
    for o in range(n_pz - 1, 0, -1):
        pl.semaphore_signal(
            barrier, inc=1, device_id={"pz": flipped(pz, o, n_pz)}, device_id_type=MESH
        )
    for o in range(n_py - 1, 0, -1):
        pl.semaphore_signal(
            barrier, inc=1, device_id={"py": flipped(py, o, n_py)}, device_id_type=MESH
        )
    load(0).start()
    sides[0].start()
    sides[1].start()
    for f in range(1, fields):
        load(f).start()
    for side in sides[2:]:
        side.start()

    def copy_y(f, o):
        to = flipped(py, o, n_py)
        return pltpu.make_async_remote_copy(
            src_ref=lines_out.at[f, to],
            dst_ref=lines.at[f, pl.ds(py * rows_y, rows_y)],
            send_sem=send_y.at[f, o],
            recv_sem=recv_y.at[f, o],
            device_id={"py": to},
            device_id_type=MESH,
        )

    near = n_pz // 2
    half = pz // near

    def across(j):
        return (1 - half) * (n_pz - 1 - j) + half * j

    def beside(o):
        return flipped(pz, o, n_pz)

    def copy_z(f, peer):
        return pltpu.make_async_remote_copy(
            src_ref=parts_out.at[f, pl.ds(peer * rows_z, rows_z)],
            dst_ref=parts.at[f, pl.ds(pz * rows_z, rows_z)],
            send_sem=send_z.at[f, peer],
            recv_sem=recv_z.at[f, pz],
            device_id={"pz": peer},
            device_id_type=MESH,
        )

    def arrival_z(f, peer):
        return pltpu.make_async_remote_copy(
            src_ref=parts_out.at[f, pl.ds(peer * rows_z, rows_z)],
            dst_ref=parts.at[f, pl.ds(peer * rows_z, rows_z)],
            send_sem=send_z.at[f, peer],
            recv_sem=recv_z.at[f, peer],
            device_id={"pz": peer},
            device_id_type=MESH,
        )

    mirror = flipped(pz, near, n_pz)
    raw_role = lax.rem(pz, 2) == 0
    plain_role = jnp.logical_not(raw_role)

    raw = pltpu.make_async_remote_copy(
        src_ref=lines_out.at[0],
        dst_ref=far,
        send_sem=send_raw.at[0],
        recv_sem=recv_raw.at[0],
        device_id={"pz": mirror},
        device_id_type=MESH,
    )

    def copy_relay(o):
        to = flipped(py, o, n_py)
        return pltpu.make_async_remote_copy(
            src_ref=far.at[to],
            dst_ref=far_lines.at[pl.ds(py * rows_y, rows_y)],
            send_sem=send_relay.at[o],
            recv_sem=recv_relay.at[o],
            device_id={"py": to},
            device_id_type=MESH,
        )

    def copy_far(o):
        to = flipped(pz, o, n_pz)
        return pltpu.make_async_remote_copy(
            src_ref=far_out.at[pl.ds((to - half * near) * rows_z, rows_z)],
            dst_ref=parts.at[0, pl.ds(mirror * rows_z, rows_z)],
            send_sem=send_far.at[o],
            recv_sem=recv_far.at[o],
            device_id={"pz": to},
            device_id_type=MESH,
        )

    for f in range(fields):
        load(f).wait()
        high, low = split(held[f])
        if f == 0:
            sides[0].wait()
            sides[1].wait()
        both = dot(jnp.concatenate([high, low], axis=0), hx[0])
        result = both[:rows_y] + both[rows_y:] + dot(high, hx[1])
        for d in range(n_py):
            lines_out[f, d] = result[:, d * share_x : (d + 1) * share_x]
        def send_lines(f):
            for o in range(n_py - 1, 0, -1):
                copy_y(f, o).start()

        if f == 0:
            pl.semaphore_wait(barrier, n_py + n_pz - 2)
            pl.when(raw_role)(raw.start)
            pl.when(plain_role)(functools.partial(send_lines, 0))
        else:
            send_lines(f)
        if f == 1:
            pl.when(raw_role)(functools.partial(send_lines, 0))
        lines[f, pl.ds(py * rows_y, rows_y)] = lines_out[f, py]

    for side in sides[2:]:
        side.wait()

    def iota(shape, dim):
        return lax.broadcasted_iota(jnp.int32, shape, dim)

    row, col = iota((depth_y, ny), 0), iota((depth_y, ny), 1)
    pick = (row // zl == col).astype(F32).astype(BF16)
    row, col = iota((ny, depth_y), 0), iota((ny, depth_y), 1)
    spread = (col // zl == row).astype(F32).astype(BF16)
    row, col = iota((depth_y, depth_y), 0), iota((depth_y, depth_y), 1)
    keep = row % zl == col % zl
    for t in range(2):
        wide = dot(dot(pick, hy[t]).astype(BF16), spread)
        my[t] = jnp.where(keep, wide, 0.0).astype(BF16)
    def rows_transform(high_table, low_table, high, low):
        both = dot(high_table, jnp.concatenate([high, low], axis=1))
        return both[:, :share_x] + both[:, share_x:] + dot(low_table, high)

    half_rows = depth_y // 2

    def send_second(f):
        for j in range(near // 2, near):
            copy_z(f, across(j)).start()

    def y_step(f, before):
        for o in range(n_py - 1, 0, -1):
            copy_y(f, o).wait_recv()
        high, low = split(lines[f])
        for h in range(2):
            part = lax.rem(half + h + 1, 2)
            span = pl.ds(pl.multiple_of(part * half_rows, half_rows), half_rows)
            parts_out[f, span] = rows_transform(my[0, span], my[1, span], high, low)
            if h == 0:
                for j in range(near // 2):
                    copy_z(f, across(j)).start()
                if before is not None:
                    send_second(before)
                if f == fields - 1:
                    send_second(f)
            else:
                for o in range(near - 1, 0, -1):
                    copy_z(f, beside(o)).start()
        parts[f, pl.ds(pz * rows_z, rows_z)] = parts_out[f, pl.ds(pz * rows_z, rows_z)]

    def relay():
        raw.wait_recv()
        for o in range(n_py - 1, 0, -1):
            copy_relay(o).start()
        far_lines[pl.ds(py * rows_y, rows_y)] = far[py]

    def near_step():
        for o in range(n_py - 1, 0, -1):
            copy_y(0, o).wait_recv()
        span = pl.ds(pl.multiple_of(half * half_rows, half_rows), half_rows)
        high, low = split(lines[0])
        parts_out[0, span] = rows_transform(my[0, span], my[1, span], high, low)
        for o in range(near - 1, 0, -1):
            copy_z(0, beside(o)).start()
        parts[0, pl.ds(pz * rows_z, rows_z)] = parts_out[0, pl.ds(pz * rows_z, rows_z)]
        for o in range(n_py - 1, 0, -1):
            copy_relay(o).wait_recv()
        high, low = split(far_lines[...])
        far_out[...] = rows_transform(my[0, span], my[1, span], high, low)
        for o in range(near - 1, 0, -1):
            copy_far(o).start()
        parts[0, pl.ds(mirror * rows_z, rows_z)] = far_out[
            pl.ds((pz - half * near) * rows_z, rows_z)
        ]

    pl.when(plain_role)(functools.partial(y_step, 0, None))
    for f in range(1, fields):
        if f == fields - 1:
            pl.when(raw_role)(near_step)
        if f == 1:
            pl.when(plain_role)(functools.partial(send_second, 0))
        y_step(f, f - 1 if f > 1 else None)
        if f == 1:
            pl.when(raw_role)(relay)

    row, col = iota((rows_out, nz), 0), iota((rows_out, nz), 1)
    pick = (row % nz == col).astype(F32).astype(BF16)
    row, col = iota((nz, depth_z), 0), iota((nz, depth_z), 1)
    spread = ((col // rows_z) * zl + col % zl == row).astype(F32).astype(BF16)
    row, col = iota((rows_out, depth_z), 0), iota((rows_out, depth_z), 1)
    keep = row // nz == (col // zl) % share_y
    for t in range(2):
        wide = dot(dot(pick, hz[t]).astype(BF16), spread)
        mz[t] = jnp.where(keep, wide, 0.0).astype(BF16)

    diagonal = iota((nz, nz), 0) == iota((nz, nz), 1)
    sz_column = jnp.sum(jnp.where(diagonal, sz[...], 0.0), axis=1, keepdims=True)
    sx_row = sx[:, pl.ds(pl.multiple_of(py * share_x, share_x), share_x)]
    for k in range(share_y):
        symbol = (sx_row + sy[pz * share_y + k]) + sz_column
        weights[pl.ds(k * nz, nz)] = 1.0 / (1.0 + symbol)

    def wait_first(role):
        for o in range(1, n_pz):
            if o % 2 == 1 - role or o < near:
                arrival_z(0, beside(o)).wait_recv()
            if o % 2 == role and o < near:
                copy_far(o).wait_recv()

    last = fields - 1
    for f in [*range(1, last), 0, last]:
        if f == 0:
            pl.when(raw_role)(functools.partial(wait_first, 0))
            pl.when(plain_role)(functools.partial(wait_first, 1))
        else:
            for o in range(1, n_pz):
                arrival_z(f, beside(o)).wait_recv()
        high, low = split(parts[f])
        if f < last:
            modes[f] = rows_transform(mz[0], mz[1], high, low)
        if f == 0:
            for k in range(share_y):
                span = pl.ds(k * nz, nz)
                weight = weights[span]
                old = [modes[b, span] for b in range(last)]
                for a in range(fields):
                    mixed = coupling[a, 0] * old[0]
                    for b in range(1, last):
                        mixed = mixed + coupling[a, b] * old[b]
                    mixed = (1.0 - weight) * mixed
                    out_ref[a, span] = mixed + weight * old[a] if a < last else mixed
        if f == last:
            result = rows_transform(mz[0], mz[1], high, low)
            weight = weights[...]
            rest = (1.0 - weight) * result
            for a in range(fields):
                new = out_ref[a] + coupling[a, last] * rest
                out_ref[a] = new + weight * result if a == last else new
    for f in range(fields):
        for o in range(1, n_py):
            copy_y(f, o).wait_send()
        for o in range(1, n_pz):
            if f or o < near:
                copy_z(f, beside(o)).wait_send()

    @pl.when(raw_role)
    def _():
        raw.wait_send()
        for o in range(1, n_py):
            copy_relay(o).wait_send()
        for o in range(1, near):
            copy_far(o).wait_send()

    @pl.when(plain_role)
    def _():
        for o in range(near, n_pz):
            copy_z(0, beside(o)).wait_send()


def shards(n_py, n_pz, species, coupling, symbol_x, symbol_y, symbol_z):
    fields, nx, yl, zl = species.shape
    ny, nz = yl * n_py, zl * n_pz
    share_x, share_y = nx // n_py, ny // n_pz
    block = fields * nx * yl * zl
    tables = 2 * (nx * nx + (ny * zl) ** 2 + (share_y * nz) ** 2)
    need = 7 * 4 * block + 2 * tables + 16 * max(ny * zl, share_y * nz) ** 2
    bad = share_x % LANES or zl % SUBLANES or nx % n_py or ny % n_pz
    if bad or need > VMEM_BUDGET or fields < 3 or n_pz % 4 or n_pz & (n_pz - 1):
        return plain_shards(species, coupling, symbol_x, symbol_y, symbol_z)
    dims = (fields, ny, nz, n_py, n_pz, yl, zl, share_x, share_y)
    rows_y, depth_y, depth_z = yl * zl, ny * zl, share_y * nz
    vmem = pl.BlockSpec(memory_space=pltpu.VMEM)
    hbm = pl.BlockSpec(memory_space=pltpu.HBM)
    values = jnp.transpose(species, (0, 2, 3, 1)).reshape(fields, rows_y, nx)
    out = pl.pallas_call(
        functools.partial(kernel, dims),
        out_shape=jax.ShapeDtypeStruct((fields, depth_z, share_x), F32),
        in_specs=[hbm] * 8,
        out_specs=vmem,
        scratch_shapes=[
            pltpu.VMEM((fields, rows_y, nx), F32),
            pltpu.VMEM((2, nx, nx), BF16),
            pltpu.VMEM((2, ny, ny), BF16),
            pltpu.VMEM((2, nz, nz), BF16),
            pltpu.SMEM((fields, fields), F32),
            pltpu.VMEM((1, nx), F32),
            pltpu.SMEM((ny,), F32),
            pltpu.VMEM((1, nz), F32),
            pltpu.VMEM((fields, n_py, rows_y, share_x), F32),
            pltpu.VMEM((fields, depth_y, share_x), F32),
            pltpu.VMEM((fields, depth_y, share_x), F32),
            pltpu.VMEM((fields, depth_z, share_x), F32),
            pltpu.VMEM((fields - 1, depth_z, share_x), F32),
            pltpu.VMEM((depth_z, share_x), F32),
            pltpu.VMEM((2, depth_y, depth_y), BF16),
            pltpu.VMEM((2, depth_z, depth_z), BF16),
            pltpu.VMEM((n_py, rows_y, share_x), F32),
            pltpu.VMEM((depth_y, share_x), F32),
            pltpu.VMEM((depth_y // 2, share_x), F32),
            pltpu.SemaphoreType.DMA((fields,)),
            pltpu.SemaphoreType.DMA((8,)),
            pltpu.SemaphoreType.DMA((fields, n_py)),
            pltpu.SemaphoreType.DMA((fields, n_py)),
            pltpu.SemaphoreType.DMA((fields, n_pz)),
            pltpu.SemaphoreType.DMA((fields, n_pz)),
            pltpu.SemaphoreType.DMA((1,)),
            pltpu.SemaphoreType.DMA((1,)),
            pltpu.SemaphoreType.DMA((n_py,)),
            pltpu.SemaphoreType.DMA((n_py,)),
            pltpu.SemaphoreType.DMA((n_pz // 2,)),
            pltpu.SemaphoreType.DMA((n_pz // 2,)),
        ],
        compiler_params=pltpu.CompilerParams(
            collective_id=0, has_side_effects=True, vmem_limit_bytes=54500000
        ),
    )(
        *(
            pltpu.with_memory_space_constraint(x, pltpu.HBM)
            for x in (
                values,
                jnp.asarray(split_table(nx)),
                jnp.asarray(split_table(ny)),
                jnp.asarray(split_table(nz)),
                coupling,
                symbol_x.reshape(1, nx),
                symbol_y,
                symbol_z.reshape(1, nz),
            )
        )
    )
    return jnp.transpose(out.reshape(fields, share_y, nz, share_x), (0, 3, 1, 2))


def solution(mesh):
    return jax.shard_map(
        functools.partial(shards, mesh.shape["py"], mesh.shape["pz"]),
        mesh=mesh,
        in_specs=(P(None, None, "py", "pz"), P(), P(), P(), P()),
        out_specs=P(None, "py", "pz", None),
        check_vma=False,
    )
```

```python
import functools

import jax
import jax.numpy as jnp
import numpy as np
from jax import lax
from jax.experimental import pallas as pl
from jax.experimental.pallas import tpu as pltpu
from jax.sharding import PartitionSpec as P

MESH = pl.DeviceIdType.MESH
F32 = jnp.float32
BF16 = jnp.bfloat16
LANES, SUBLANES = 128, 8
VMEM_BUDGET = 48 << 20


def mode_table(count):
    rank = jnp.arange(count)
    angle = (
        jnp.pi
        / (4 * count)
        * ((2 * rank[:, None] + 1) * (2 * rank[None, :] + 1) % (8 * count)).astype(jnp.float32)
    )
    return jnp.cos(angle) * (2.0 / count) ** 0.5


def transform_dim(values, dim):
    moved = jnp.tensordot(
        values, mode_table(values.shape[dim]), axes=([dim], [0]), precision=lax.Precision.HIGHEST
    )
    return jnp.moveaxis(moved, -1, dim)


def plain_shards(species, coupling, symbol_x, symbol_y, symbol_z):
    values = transform_dim(species, 1)
    values = lax.all_to_all(values, "py", split_axis=1, concat_axis=2, tiled=True)
    values = transform_dim(values, 2)
    values = lax.all_to_all(values, "pz", split_axis=2, concat_axis=3, tiled=True)
    values = transform_dim(values, 3)
    share_x = values.shape[1]
    part_x = lax.dynamic_slice_in_dim(symbol_x, lax.axis_index("py") * share_x, share_x)
    share_y = values.shape[2]
    part_y = lax.dynamic_slice_in_dim(symbol_y, lax.axis_index("pz") * share_y, share_y)
    symbol = part_x[:, None, None] + part_y[None, :, None] + symbol_z[None, None, :]
    weight = 1.0 / (1.0 + symbol)
    mixed = jnp.einsum("ab,bxyz->axyz", coupling, values, precision=lax.Precision.HIGHEST)
    return weight * values + (1.0 - weight) * mixed


def split_table(count):
    rank = 2 * np.arange(count) + 1
    table = np.cos(np.pi / (4 * count) * (rank[:, None] * rank[None, :] % (8 * count)))
    table = (table * np.sqrt(2.0 / count)).astype(np.float32)
    high = table.astype(BF16)
    low = (table - high.astype(np.float32)).astype(BF16)
    return np.stack([high, low])


def split(values):
    high = values.astype(BF16)
    low = (values - high.astype(F32)).astype(BF16)
    return high, low


def dot(a, b):
    return jnp.dot(a, b, preferred_element_type=F32)


def flipped(index, offset, count):
    if count & (count - 1):
        return lax.rem(index + offset, count)
    result = index
    bit = 1
    while bit < count:
        if offset & bit:
            result = result + bit - 2 * bit * lax.rem(index // bit, 2)
        bit *= 2
    return result


def source_of(index, offset, count):
    if count & (count - 1):
        return lax.rem(index + count - offset, count)
    return flipped(index, offset, count)


def kernel(
    dims, field_ref, hx_hbm, hy_hbm, hz_hbm, coupling_hbm, sx_hbm, sy_hbm, sz_hbm, out_ref,
    held, hx, hy, hz, coupling, sx, sy, sz, lines_out, lines, parts_out, parts, modes, weights,
    my, mz, far, far_lines, far_out, load_sem, side_sem, send_y, recv_y, send_z, recv_z,
    send_raw, recv_raw, send_relay, recv_relay, send_far,
):
    fields, ny, nz, n_py, n_pz, yl, zl, share_x, share_y = dims
    py, pz = lax.axis_index("py"), lax.axis_index("pz")
    rows_y = yl * zl
    rows_z = share_y * zl
    depth_y = ny * zl
    group = max(g for g in range(1, share_y + 1) if share_y % g == 0 and g * nz <= max(nz, 256))
    rows_g, rows_out = group * zl, group * nz
    depth_g = n_pz * rows_g

    def load(f):
        return pltpu.make_async_copy(field_ref.at[f], held.at[f], load_sem.at[f])

    pairs = (
        (hx_hbm, hx), (hy_hbm, hy), (hz_hbm, hz),
        (coupling_hbm, coupling), (sx_hbm, sx), (sy_hbm, sy), (sz_hbm, sz),
    )
    sides = [
        pltpu.make_async_copy(a, b, side_sem.at[i]) for i, (a, b) in enumerate(pairs)
    ]
    barrier = pltpu.get_barrier_semaphore()
    for o in range(n_pz - 1, 0, -1):
        pl.semaphore_signal(
            barrier, inc=1, device_id={"pz": flipped(pz, o, n_pz)}, device_id_type=MESH
        )
    for o in range(n_py - 1, 0, -1):
        pl.semaphore_signal(
            barrier, inc=1, device_id={"py": flipped(py, o, n_py)}, device_id_type=MESH
        )
    load(0).start()
    sides[0].start()
    for f in range(1, fields):
        load(f).start()
    for side in sides[1:]:
        side.start()

    def copy_y(f, o):
        to = flipped(py, o, n_py)
        return pltpu.make_async_remote_copy(
            src_ref=lines_out.at[f, to],
            dst_ref=lines.at[f, pl.ds(py * rows_y, rows_y)],
            send_sem=send_y.at[f],
            recv_sem=recv_y.at[f],
            device_id={"py": to},
            device_id_type=MESH,
        )

    near = n_pz // 2
    half = pz // near

    def across(j):
        return (1 - half) * (n_pz - 1 - j) + half * j

    def beside(o):
        return flipped(pz, o, n_pz)

    def copy_z(f, peer, piece=None):
        rows, first = (rows_z, 0) if piece is None else (rows_g, piece * rows_g)
        return pltpu.make_async_remote_copy(
            src_ref=parts_out.at[f, pl.ds(peer * rows_z + first, rows)],
            dst_ref=parts.at[f, pl.ds(pz * rows_z + first, rows)],
            send_sem=send_z.at[f],
            recv_sem=recv_z.at[f if piece is None else f + piece],
            device_id={"pz": peer},
            device_id_type=MESH,
        )

    def wait_for(ref, sem):
        pltpu.make_async_copy(ref, ref, sem).wait()

    def wait_lines(f):
        wait_for(lines.at[f, pl.ds(0, (n_py - 1) * rows_y)], recv_y.at[f])

    mirror = flipped(pz, near, n_pz)
    raw_role = lax.rem(pz, 2) == 0
    plain_role = jnp.logical_not(raw_role)

    raw = pltpu.make_async_remote_copy(
        src_ref=lines_out.at[0],
        dst_ref=far,
        send_sem=send_raw.at[0],
        recv_sem=recv_raw.at[0],
        device_id={"pz": mirror},
        device_id_type=MESH,
    )

    def copy_relay(o):
        to = flipped(py, o, n_py)
        return pltpu.make_async_remote_copy(
            src_ref=far.at[to],
            dst_ref=far_lines.at[pl.ds(py * rows_y, rows_y)],
            send_sem=send_relay.at[0],
            recv_sem=recv_relay.at[0],
            device_id={"py": to},
            device_id_type=MESH,
        )

    def copy_far(o):
        to = flipped(pz, o, n_pz)
        return pltpu.make_async_remote_copy(
            src_ref=far_out.at[pl.ds((to - half * near) * rows_z, rows_z)],
            dst_ref=parts.at[0, pl.ds(mirror * rows_z, rows_z)],
            send_sem=send_far.at[0],
            recv_sem=recv_z.at[0],
            device_id={"pz": to},
            device_id_type=MESH,
        )

    for f in range(fields):
        load(f).wait()
        high, low = split(held[f])
        if f == 0:
            sides[0].wait()
        both = dot(jnp.concatenate([high, low], axis=0), hx[0])
        result = both[:rows_y] + both[rows_y:] + dot(high, hx[1])
        for d in range(n_py):
            lines_out[f, d] = result[:, d * share_x : (d + 1) * share_x]
        def send_lines(f):
            for o in range(n_py - 1, 0, -1):
                copy_y(f, o).start()

        if f == 0:
            pl.semaphore_wait(barrier, n_py + n_pz - 2)
            pl.when(raw_role)(raw.start)
            pl.when(plain_role)(functools.partial(send_lines, 0))
        else:
            send_lines(f)
        if f == 1:
            pl.when(raw_role)(functools.partial(send_lines, 0))
        lines[f, pl.ds(py * rows_y, rows_y)] = lines_out[f, py]

    for side in sides[1:]:
        side.wait()

    def iota(shape, dim):
        return lax.broadcasted_iota(jnp.int32, shape, dim)

    row, col = iota((depth_y, ny), 0), iota((depth_y, ny), 1)
    pick = (row // zl == col).astype(F32).astype(BF16)
    row, col = iota((ny, depth_y), 0), iota((ny, depth_y), 1)
    spread = (col // zl == row).astype(F32).astype(BF16)
    row, col = iota((depth_y, depth_y), 0), iota((depth_y, depth_y), 1)
    keep = row % zl == col % zl
    for t in range(2):
        wide = dot(dot(pick, hy[t]).astype(BF16), spread)
        my[t] = jnp.where(keep, wide, 0.0).astype(BF16)
    def rows_transform(high_table, low_table, high, low):
        both = dot(high_table, jnp.concatenate([high, low], axis=1))
        return both[:, :share_x] + both[:, share_x:] + dot(low_table, high)

    half_rows = depth_y // 2

    last = fields - 1
    pieces = share_y // group

    def send_parts(f, peers):
        for piece in range(pieces) if f == last else [None]:
            for peer in peers:
                copy_z(f, peer, piece).start()

    outer = [across(j) for j in range(near // 2)]
    inner = [across(j) for j in range(near // 2, near)]
    around = [beside(o) for o in range(near - 1, 0, -1)]

    def y_step(f, before):
        wait_lines(f)
        high, low = split(lines[f])
        for h in range(2):
            part = lax.rem(half + h + 1, 2)
            span = pl.ds(pl.multiple_of(part * half_rows, half_rows), half_rows)
            parts_out[f, span] = rows_transform(my[0, span], my[1, span], high, low)
            if h == 0:
                send_parts(f, outer)
                if before is not None:
                    send_parts(before, inner)
                if f == last:
                    send_parts(f, inner)
            else:
                send_parts(f, around)
        parts[f, pl.ds(pz * rows_z, rows_z)] = parts_out[f, pl.ds(pz * rows_z, rows_z)]

    def relay():
        raw.wait_recv()
        for o in range(n_py - 1, 0, -1):
            copy_relay(o).start()
        far_lines[pl.ds(py * rows_y, rows_y)] = far[py]

    def near_step():
        wait_lines(0)
        span = pl.ds(pl.multiple_of(half * half_rows, half_rows), half_rows)
        high, low = split(lines[0])
        parts_out[0, span] = rows_transform(my[0, span], my[1, span], high, low)
        send_parts(0, around)
        parts[0, pl.ds(pz * rows_z, rows_z)] = parts_out[0, pl.ds(pz * rows_z, rows_z)]
        wait_for(far_lines.at[pl.ds(0, (n_py - 1) * rows_y)], recv_relay.at[0])
        high, low = split(far_lines[...])
        far_out[...] = rows_transform(my[0, span], my[1, span], high, low)
        for o in range(near - 1, 0, -1):
            copy_far(o).start()
        parts[0, pl.ds(mirror * rows_z, rows_z)] = far_out[
            pl.ds((pz - half * near) * rows_z, rows_z)
        ]

    pl.when(plain_role)(functools.partial(y_step, 0, None))
    for f in range(1, fields):
        if f == fields - 1:
            pl.when(raw_role)(near_step)
        if f == 1:
            pl.when(plain_role)(functools.partial(send_parts, 0, inner))
        y_step(f, f - 1 if f > 1 else None)
        if f == 1:
            pl.when(raw_role)(relay)

    row, col = iota((rows_out, nz), 0), iota((rows_out, nz), 1)
    pick = (row % nz == col).astype(F32).astype(BF16)
    row, col = iota((nz, depth_g), 0), iota((nz, depth_g), 1)
    spread = ((col // rows_g) * zl + col % zl == row).astype(F32).astype(BF16)
    row, col = iota((rows_out, depth_g), 0), iota((rows_out, depth_g), 1)
    keep = row // nz == (col // zl) % group
    for t in range(2):
        wide = dot(dot(pick, hz[t]).astype(BF16), spread)
        mz[t] = jnp.where(keep, wide, 0.0).astype(BF16)

    def z_step(f, g):
        starts = [p * rows_z + g * rows_g for p in range(n_pz)]
        block = jnp.concatenate([parts[f, a : a + rows_g] for a in starts], axis=0)
        return rows_transform(mz[0], mz[1], *split(block))

    diagonal = iota((nz, nz), 0) == iota((nz, nz), 1)
    sz_column = jnp.sum(jnp.where(diagonal, sz[...], 0.0), axis=1, keepdims=True)
    sx_row = sx[:, pl.ds(pl.multiple_of(py * share_x, share_x), share_x)]
    for k in range(share_y):
        symbol = (sx_row + sy[pz * share_y + k]) + sz_column
        weights[pl.ds(k * nz, nz)] = 1.0 / (1.0 + symbol)

    def wait_parts(f, blocks):
        wait_for(parts.at[f, pl.ds(0, blocks * rows_z)], recv_z.at[f])

    for f in [*range(1, last), 0, last]:
        if f == 0:
            pl.when(raw_role)(functools.partial(wait_parts, 0, n_pz - 2))
            pl.when(plain_role)(functools.partial(wait_parts, 0, n_pz - 1))
        elif f < last:
            wait_parts(f, n_pz - 1)
        if f < last:
            for g in range(pieces):
                modes[f, pl.ds(g * rows_out, rows_out)] = z_step(f, g)
        if f == 0:
            for k in range(share_y):
                span = pl.ds(k * nz, nz)
                weight = weights[span]
                old = [modes[b, span] for b in range(last)]
                for a in range(fields):
                    mixed = coupling[a, 0] * old[0]
                    for b in range(1, last):
                        mixed = mixed + coupling[a, b] * old[b]
                    mixed = (1.0 - weight) * mixed
                    out_ref[a, span] = mixed + weight * old[a] if a < last else mixed
        if f == last:
            for g in range(pieces):
                wait_for(parts.at[f, pl.ds(0, (n_pz - 1) * rows_g)], recv_z.at[f + g])
                span = pl.ds(g * rows_out, rows_out)
                result = z_step(f, g)
                weight = weights[span]
                rest = (1.0 - weight) * result
                for a in range(fields):
                    new = out_ref[a, span] + coupling[a, last] * rest
                    out_ref[a, span] = new + weight * result if a == last else new
    def sent_parts(f, blocks):
        wait_for(parts_out.at[f, pl.ds(0, blocks * rows_z)], send_z.at[f])

    for f in range(fields):
        wait_for(lines_out.at[f, pl.ds(0, n_py - 1)], send_y.at[f])
        if f:
            sent_parts(f, n_pz - 1)

    @pl.when(raw_role)
    def _():
        raw.wait_send()
        wait_for(far.at[pl.ds(0, n_py - 1)], send_relay.at[0])
        wait_for(far_out.at[pl.ds(0, (near - 1) * rows_z)], send_far.at[0])
        sent_parts(0, near - 1)

    @pl.when(plain_role)
    def _():
        sent_parts(0, n_pz - 1)


def shards(n_py, n_pz, species, coupling, symbol_x, symbol_y, symbol_z):
    fields, nx, yl, zl = species.shape
    ny, nz = yl * n_py, zl * n_pz
    share_x, share_y = nx // n_py, ny // n_pz
    block = fields * nx * yl * zl
    tables = 2 * (nx * nx + (ny * zl) ** 2 + (share_y * nz) ** 2)
    need = 7 * 4 * block + 2 * tables + 16 * max(ny * zl, share_y * nz) ** 2
    bad = share_x % LANES or zl % SUBLANES or nx % n_py or ny % n_pz
    if bad or need > VMEM_BUDGET or fields < 3 or n_pz % 4 or n_pz & (n_pz - 1):
        return plain_shards(species, coupling, symbol_x, symbol_y, symbol_z)
    dims = (fields, ny, nz, n_py, n_pz, yl, zl, share_x, share_y)
    rows_y, depth_y, depth_z = yl * zl, ny * zl, share_y * nz
    width = nz * max(g for g in range(1, share_y + 1) if share_y % g == 0 and g * nz <= max(nz, 256))
    vmem = pl.BlockSpec(memory_space=pltpu.VMEM)
    hbm = pl.BlockSpec(memory_space=pltpu.HBM)
    values = jnp.transpose(species, (0, 2, 3, 1)).reshape(fields, rows_y, nx)
    out = pl.pallas_call(
        functools.partial(kernel, dims),
        out_shape=jax.ShapeDtypeStruct((fields, depth_z, share_x), F32),
        in_specs=[hbm] * 8,
        out_specs=vmem,
        scratch_shapes=[
            pltpu.VMEM((fields, rows_y, nx), F32),
            pltpu.VMEM((2, nx, nx), BF16),
            pltpu.VMEM((2, ny, ny), BF16),
            pltpu.VMEM((2, nz, nz), BF16),
            pltpu.SMEM((fields, fields), F32),
            pltpu.VMEM((1, nx), F32),
            pltpu.SMEM((ny,), F32),
            pltpu.VMEM((1, nz), F32),
            pltpu.VMEM((fields, n_py, rows_y, share_x), F32),
            pltpu.VMEM((fields, depth_y, share_x), F32),
            pltpu.VMEM((fields, depth_y, share_x), F32),
            pltpu.VMEM((fields, depth_z, share_x), F32),
            pltpu.VMEM((fields - 1, depth_z, share_x), F32),
            pltpu.VMEM((depth_z, share_x), F32),
            pltpu.VMEM((2, depth_y, depth_y), BF16),
            pltpu.VMEM((2, width, width), BF16),
            pltpu.VMEM((n_py, rows_y, share_x), F32),
            pltpu.VMEM((depth_y, share_x), F32),
            pltpu.VMEM((depth_y // 2, share_x), F32),
            pltpu.SemaphoreType.DMA((fields,)),
            pltpu.SemaphoreType.DMA((7,)),
            pltpu.SemaphoreType.DMA((fields,)),
            pltpu.SemaphoreType.DMA((fields,)),
            pltpu.SemaphoreType.DMA((fields,)),
            pltpu.SemaphoreType.DMA((fields + share_y * nz // width - 1,)),
            pltpu.SemaphoreType.DMA((1,)),
            pltpu.SemaphoreType.DMA((1,)),
            pltpu.SemaphoreType.DMA((1,)),
            pltpu.SemaphoreType.DMA((1,)),
            pltpu.SemaphoreType.DMA((1,)),
        ],
        compiler_params=pltpu.CompilerParams(
            collective_id=0, has_side_effects=True, vmem_limit_bytes=54500000
        ),
    )(
        *(
            pltpu.with_memory_space_constraint(x, pltpu.HBM)
            for x in (
                values,
                jnp.asarray(split_table(nx)),
                jnp.asarray(split_table(ny)),
                jnp.asarray(split_table(nz)),
                coupling,
                symbol_x.reshape(1, nx),
                symbol_y,
                symbol_z.reshape(1, nz),
            )
        )
    )
    return jnp.transpose(out.reshape(fields, share_y, nz, share_x), (0, 3, 1, 2))


def solution(mesh):
    return jax.shard_map(
        functools.partial(shards, mesh.shape["py"], mesh.shape["pz"]),
        mesh=mesh,
        in_specs=(P(None, None, "py", "pz"), P(), P(), P(), P()),
        out_specs=P(None, "py", "pz", None),
        check_vma=False,
    )
```

```python
import functools

import jax
import jax.numpy as jnp
import numpy as np
from jax import lax
from jax.experimental import pallas as pl
from jax.experimental.pallas import tpu as pltpu
from jax.sharding import PartitionSpec as P

MESH = pl.DeviceIdType.MESH
F32 = jnp.float32
BF16 = jnp.bfloat16
LANES, SUBLANES = 128, 8
VMEM_BUDGET = 48 << 20
RAW_SHARES = ((0, 1, 2), (0, 1, 3))


def mode_table(count):
    rank = jnp.arange(count)
    angle = (
        jnp.pi
        / (4 * count)
        * ((2 * rank[:, None] + 1) * (2 * rank[None, :] + 1) % (8 * count)).astype(jnp.float32)
    )
    return jnp.cos(angle) * (2.0 / count) ** 0.5


def transform_dim(values, dim):
    moved = jnp.tensordot(
        values, mode_table(values.shape[dim]), axes=([dim], [0]), precision=lax.Precision.HIGHEST
    )
    return jnp.moveaxis(moved, -1, dim)


def plain_shards(species, coupling, symbol_x, symbol_y, symbol_z):
    values = transform_dim(species, 1)
    values = lax.all_to_all(values, "py", split_axis=1, concat_axis=2, tiled=True)
    values = transform_dim(values, 2)
    values = lax.all_to_all(values, "pz", split_axis=2, concat_axis=3, tiled=True)
    values = transform_dim(values, 3)
    share_x = values.shape[1]
    part_x = lax.dynamic_slice_in_dim(symbol_x, lax.axis_index("py") * share_x, share_x)
    share_y = values.shape[2]
    part_y = lax.dynamic_slice_in_dim(symbol_y, lax.axis_index("pz") * share_y, share_y)
    symbol = part_x[:, None, None] + part_y[None, :, None] + symbol_z[None, None, :]
    weight = 1.0 / (1.0 + symbol)
    mixed = jnp.einsum("ab,bxyz->axyz", coupling, values, precision=lax.Precision.HIGHEST)
    return weight * values + (1.0 - weight) * mixed


def split_table(count):
    rank = 2 * np.arange(count) + 1
    table = np.cos(np.pi / (4 * count) * (rank[:, None] * rank[None, :] % (8 * count)))
    table = (table * np.sqrt(2.0 / count)).astype(np.float32)
    high = table.astype(BF16)
    low = (table - high.astype(np.float32)).astype(BF16)
    return np.stack([high, low])


def split(values):
    high = values.astype(BF16)
    low = (values - high.astype(F32)).astype(BF16)
    return high, low


def dot(a, b):
    return jnp.dot(a, b, preferred_element_type=F32)


def flipped(index, offset, count):
    if count & (count - 1):
        return lax.rem(index + offset, count)
    result = index
    bit = 1
    while bit < count:
        if offset & bit:
            result = result + bit - 2 * bit * lax.rem(index // bit, 2)
        bit *= 2
    return result


def source_of(index, offset, count):
    if count & (count - 1):
        return lax.rem(index + count - offset, count)
    return flipped(index, offset, count)


def kernel(
    dims, field_ref, hx_hbm, hy_hbm, hz_hbm, coupling_hbm, sx_hbm, sy_hbm, sz_hbm, out_ref,
    held, hx, hy, hz, coupling, sx, sy, sz, lines_out, lines, parts_out, parts, modes, weights,
    my, mz, far, far_lines, far_out, load_sem, side_sem, send_y, recv_y, send_z, recv_z,
    send_raw, recv_raw, send_relay, recv_relay, send_far,
):
    fields, ny, nz, n_py, n_pz, yl, zl, share_x, share_y = dims
    py, pz = lax.axis_index("py"), lax.axis_index("pz")
    rows_y = yl * zl
    rows_z = share_y * zl
    depth_y = ny * zl
    group = max(g for g in range(1, share_y + 1) if share_y % g == 0 and g * nz <= max(nz, 256))
    rows_g, rows_out = group * zl, group * nz
    depth_g = n_pz * rows_g

    def load(f):
        return pltpu.make_async_copy(field_ref.at[f], held.at[f], load_sem.at[f])

    pairs = (
        (hx_hbm, hx), (hy_hbm, hy), (hz_hbm, hz),
        (coupling_hbm, coupling), (sx_hbm, sx), (sy_hbm, sy), (sz_hbm, sz),
    )
    sides = [
        pltpu.make_async_copy(a, b, side_sem.at[i]) for i, (a, b) in enumerate(pairs)
    ]
    barrier = pltpu.get_barrier_semaphore()
    for o in range(n_pz - 1, 0, -1):
        pl.semaphore_signal(
            barrier, inc=1, device_id={"pz": flipped(pz, o, n_pz)}, device_id_type=MESH
        )
    for o in range(n_py - 1, 0, -1):
        pl.semaphore_signal(
            barrier, inc=1, device_id={"py": flipped(py, o, n_py)}, device_id_type=MESH
        )
    load(0).start()
    sides[0].start()
    for f in range(1, fields):
        load(f).start()
    for side in sides[1:]:
        side.start()

    def copy_y(f, o):
        to = flipped(py, o, n_py)
        return pltpu.make_async_remote_copy(
            src_ref=lines_out.at[f, to],
            dst_ref=lines.at[f, pl.ds(py * rows_y, rows_y)],
            send_sem=send_y.at[f],
            recv_sem=recv_y.at[f],
            device_id={"py": to},
            device_id_type=MESH,
        )

    near = n_pz // 2
    half = pz // near

    def across(j):
        return (1 - half) * (n_pz - 1 - j) + half * j

    def beside(o):
        return flipped(pz, o, n_pz)

    def copy_z(f, peer, piece=None):
        rows, first = (rows_z, 0) if piece is None else (rows_g, piece * rows_g)
        return pltpu.make_async_remote_copy(
            src_ref=parts_out.at[f, pl.ds(peer * rows_z + first, rows)],
            dst_ref=parts.at[f, pl.ds(pz * rows_z + first, rows)],
            send_sem=send_z.at[f],
            recv_sem=recv_z.at[f if piece is None else f + piece],
            device_id={"pz": peer},
            device_id_type=MESH,
        )

    def wait_for(ref, sem):
        pltpu.make_async_copy(ref, ref, sem).wait()

    def wait_lines(f):
        wait_for(lines.at[f, pl.ds(0, (n_py - 1) * rows_y)], recv_y.at[f])

    mirror = flipped(pz, near, n_pz)
    early = lax.rem(pz, 2) == 0
    pair = lax.rem(pz // 2, 2)

    def is_raw(share):
        found = jnp.bool_(False)
        for bit, shares in enumerate(RAW_SHARES):
            for s in shares:
                found = found | ((pair == bit) & (share == s))
        return early & found

    raw_role = is_raw(py)
    plain_role = jnp.logical_not(raw_role)

    def each_pair(do):
        for bit, shares in enumerate(RAW_SHARES):
            pl.when(early & (pair == bit))(functools.partial(do, shares))

    def copy_raw(share):
        return pltpu.make_async_remote_copy(
            src_ref=lines_out.at[0, share],
            dst_ref=far.at[share],
            send_sem=send_raw.at[0],
            recv_sem=recv_raw.at[0],
            device_id={"pz": mirror},
            device_id_type=MESH,
        )

    def send_raws(shares):
        for share in shares:
            copy_raw(share).start()

    def copy_relay(o):
        to = flipped(py, o, n_py)
        return pltpu.make_async_remote_copy(
            src_ref=far.at[to],
            dst_ref=far_lines.at[pl.ds(py * rows_y, rows_y)],
            send_sem=send_relay.at[o],
            recv_sem=recv_relay.at[0],
            device_id={"py": to},
            device_id_type=MESH,
        )

    def copy_far(o):
        to = flipped(pz, o, n_pz)
        return pltpu.make_async_remote_copy(
            src_ref=far_out.at[pl.ds((to - half * near) * rows_z, rows_z)],
            dst_ref=parts.at[0, pl.ds(mirror * rows_z, rows_z)],
            send_sem=send_far.at[0],
            recv_sem=recv_z.at[0],
            device_id={"pz": to},
            device_id_type=MESH,
        )

    for f in range(fields):
        load(f).wait()
        high, low = split(held[f])
        if f == 0:
            sides[0].wait()
        both = dot(jnp.concatenate([high, low], axis=0), hx[0])
        result = both[:rows_y] + both[rows_y:] + dot(high, hx[1])
        for d in range(n_py):
            lines_out[f, d] = result[:, d * share_x : (d + 1) * share_x]
        def send_lines(f, when=None):
            for o in range(n_py - 1, 0, -1):
                start = copy_y(f, o).start
                if when is None:
                    start()
                else:
                    pl.when(is_raw(flipped(py, o, n_py)) == when)(start)

        if f == 0:
            pl.semaphore_wait(barrier, n_py + n_pz - 2)
            each_pair(send_raws)
            send_lines(0, False)
        elif f == 1:
            pl.when(jnp.logical_not(early))(functools.partial(send_lines, 1))
        else:
            if f == 2:
                pl.when(early)(functools.partial(send_lines, 1))
                send_lines(0, True)
            send_lines(f)
        lines[f, pl.ds(py * rows_y, rows_y)] = lines_out[f, py]

    for side in sides[1:]:
        side.wait()

    def iota(shape, dim):
        return lax.broadcasted_iota(jnp.int32, shape, dim)

    row, col = iota((depth_y, ny), 0), iota((depth_y, ny), 1)
    pick = (row // zl == col).astype(F32).astype(BF16)
    row, col = iota((ny, depth_y), 0), iota((ny, depth_y), 1)
    spread = (col // zl == row).astype(F32).astype(BF16)
    row, col = iota((depth_y, depth_y), 0), iota((depth_y, depth_y), 1)
    keep = row % zl == col % zl
    for t in range(2):
        wide = dot(dot(pick, hy[t]).astype(BF16), spread)
        my[t] = jnp.where(keep, wide, 0.0).astype(BF16)
    def rows_transform(high_table, low_table, high, low):
        both = dot(high_table, jnp.concatenate([high, low], axis=1))
        return both[:, :share_x] + both[:, share_x:] + dot(low_table, high)

    half_rows = depth_y // 2

    last = fields - 1
    pieces = share_y // group

    def send_parts(f, peers):
        for piece in range(pieces) if f == last else [None]:
            for peer in peers:
                copy_z(f, peer, piece).start()

    outer = [across(j) for j in range(near // 2)]
    inner = [across(j) for j in range(near // 2, near)]
    around = [beside(o) for o in range(near - 1, 0, -1)]

    def y_step(f, before):
        wait_lines(f)
        high, low = split(lines[f])
        for h in range(2):
            part = lax.rem(half + h + 1, 2)
            span = pl.ds(pl.multiple_of(part * half_rows, half_rows), half_rows)
            parts_out[f, span] = rows_transform(my[0, span], my[1, span], high, low)
            if h == 0:
                send_parts(f, outer)
                if before is not None:
                    send_parts(before, inner)
                if f == last:
                    send_parts(f, inner)
            else:
                send_parts(f, around)
        parts[f, pl.ds(pz * rows_z, rows_z)] = parts_out[f, pl.ds(pz * rows_z, rows_z)]

    def relay():
        each_pair(lambda shares: wait_for(far.at[pl.ds(0, len(shares))], recv_raw.at[0]))
        for o in range(n_py - 1, 0, -1):
            pl.when(is_raw(flipped(py, o, n_py)))(copy_relay(o).start)

        @pl.when(raw_role)
        def _():
            far_lines[pl.ds(py * rows_y, rows_y)] = far[py]

    def near_step():
        wait_lines(0)
        span = pl.ds(pl.multiple_of(half * half_rows, half_rows), half_rows)
        high, low = split(lines[0])
        parts_out[0, span] = rows_transform(my[0, span], my[1, span], high, low)
        send_parts(0, around)
        parts[0, pl.ds(pz * rows_z, rows_z)] = parts_out[0, pl.ds(pz * rows_z, rows_z)]
        wait_for(far_lines.at[pl.ds(0, (n_py - 1) * rows_y)], recv_relay.at[0])
        high, low = split(far_lines[...])
        far_out[...] = rows_transform(my[0, span], my[1, span], high, low)
        for o in range(near - 1, 0, -1):
            copy_far(o).start()
        parts[0, pl.ds(mirror * rows_z, rows_z)] = far_out[
            pl.ds((pz - half * near) * rows_z, rows_z)
        ]

    pl.when(plain_role)(functools.partial(y_step, 0, None))
    for f in range(1, fields):
        if f == fields - 1:
            pl.when(raw_role)(near_step)
        if f == 1:
            pl.when(plain_role)(functools.partial(send_parts, 0, inner))
        y_step(f, f - 1 if f > 1 else None)
        if f == 1:
            relay()

    row, col = iota((rows_out, nz), 0), iota((rows_out, nz), 1)
    pick = (row % nz == col).astype(F32).astype(BF16)
    row, col = iota((nz, depth_g), 0), iota((nz, depth_g), 1)
    spread = ((col // rows_g) * zl + col % zl == row).astype(F32).astype(BF16)
    row, col = iota((rows_out, depth_g), 0), iota((rows_out, depth_g), 1)
    keep = row // nz == (col // zl) % group
    for t in range(2):
        wide = dot(dot(pick, hz[t]).astype(BF16), spread)
        mz[t] = jnp.where(keep, wide, 0.0).astype(BF16)

    def z_step(f, g):
        starts = [p * rows_z + g * rows_g for p in range(n_pz)]
        block = jnp.concatenate([parts[f, a : a + rows_g] for a in starts], axis=0)
        return rows_transform(mz[0], mz[1], *split(block))

    diagonal = iota((nz, nz), 0) == iota((nz, nz), 1)
    sz_column = jnp.sum(jnp.where(diagonal, sz[...], 0.0), axis=1, keepdims=True)
    sx_row = sx[:, pl.ds(pl.multiple_of(py * share_x, share_x), share_x)]
    for k in range(share_y):
        symbol = (sx_row + sy[pz * share_y + k]) + sz_column
        weights[pl.ds(k * nz, nz)] = 1.0 / (1.0 + symbol)

    def wait_parts(f, blocks):
        wait_for(parts.at[f, pl.ds(0, blocks * rows_z)], recv_z.at[f])

    for f in [*range(1, last), 0, last]:
        if f == 0:
            pl.when(raw_role)(functools.partial(wait_parts, 0, n_pz - 2))
            pl.when(plain_role)(functools.partial(wait_parts, 0, n_pz - 1))
        elif f < last:
            wait_parts(f, n_pz - 1)
        if f < last:
            for g in range(pieces):
                modes[f, pl.ds(g * rows_out, rows_out)] = z_step(f, g)
        if f == 0:
            for k in range(share_y):
                span = pl.ds(k * nz, nz)
                weight = weights[span]
                old = [modes[b, span] for b in range(last)]
                for a in range(fields):
                    mixed = coupling[a, 0] * old[0]
                    for b in range(1, last):
                        mixed = mixed + coupling[a, b] * old[b]
                    mixed = (1.0 - weight) * mixed
                    out_ref[a, span] = mixed + weight * old[a] if a < last else mixed
        if f == last:
            for g in range(pieces):
                wait_for(parts.at[f, pl.ds(0, (n_pz - 1) * rows_g)], recv_z.at[f + g])
                span = pl.ds(g * rows_out, rows_out)
                result = z_step(f, g)
                weight = weights[span]
                rest = (1.0 - weight) * result
                for a in range(fields):
                    new = out_ref[a, span] + coupling[a, last] * rest
                    out_ref[a, span] = new + weight * result if a == last else new
    def sent_parts(f, blocks):
        wait_for(parts_out.at[f, pl.ds(0, blocks * rows_z)], send_z.at[f])

    for f in range(fields):
        wait_for(lines_out.at[f, pl.ds(0, n_py - 1)], send_y.at[f])
        if f:
            sent_parts(f, n_pz - 1)

    each_pair(lambda shares: wait_for(far.at[pl.ds(0, len(shares))], send_raw.at[0]))
    for o in range(1, n_py):
        pl.when(is_raw(flipped(py, o, n_py)))(copy_relay(o).wait_send)

    @pl.when(raw_role)
    def _():
        wait_for(far_out.at[pl.ds(0, (near - 1) * rows_z)], send_far.at[0])
        sent_parts(0, near - 1)

    @pl.when(plain_role)
    def _():
        sent_parts(0, n_pz - 1)


def shards(n_py, n_pz, species, coupling, symbol_x, symbol_y, symbol_z):
    fields, nx, yl, zl = species.shape
    ny, nz = yl * n_py, zl * n_pz
    share_x, share_y = nx // n_py, ny // n_pz
    block = fields * nx * yl * zl
    tables = 2 * (nx * nx + (ny * zl) ** 2 + (share_y * nz) ** 2)
    need = 7 * 4 * block + 2 * tables + 16 * max(ny * zl, share_y * nz) ** 2
    bad = share_x % LANES or zl % SUBLANES or nx % n_py or ny % n_pz
    if bad or need > VMEM_BUDGET or fields < 3 or n_pz % 4 or n_pz & (n_pz - 1):
        return plain_shards(species, coupling, symbol_x, symbol_y, symbol_z)
    dims = (fields, ny, nz, n_py, n_pz, yl, zl, share_x, share_y)
    rows_y, depth_y, depth_z = yl * zl, ny * zl, share_y * nz
    width = nz * max(g for g in range(1, share_y + 1) if share_y % g == 0 and g * nz <= max(nz, 256))
    vmem = pl.BlockSpec(memory_space=pltpu.VMEM)
    hbm = pl.BlockSpec(memory_space=pltpu.HBM)
    values = jnp.transpose(species, (0, 2, 3, 1)).reshape(fields, rows_y, nx)
    out = pl.pallas_call(
        functools.partial(kernel, dims),
        out_shape=jax.ShapeDtypeStruct((fields, depth_z, share_x), F32),
        in_specs=[hbm] * 8,
        out_specs=vmem,
        scratch_shapes=[
            pltpu.VMEM((fields, rows_y, nx), F32),
            pltpu.VMEM((2, nx, nx), BF16),
            pltpu.VMEM((2, ny, ny), BF16),
            pltpu.VMEM((2, nz, nz), BF16),
            pltpu.SMEM((fields, fields), F32),
            pltpu.VMEM((1, nx), F32),
            pltpu.SMEM((ny,), F32),
            pltpu.VMEM((1, nz), F32),
            pltpu.VMEM((fields, n_py, rows_y, share_x), F32),
            pltpu.VMEM((fields, depth_y, share_x), F32),
            pltpu.VMEM((fields, depth_y, share_x), F32),
            pltpu.VMEM((fields, depth_z, share_x), F32),
            pltpu.VMEM((fields - 1, depth_z, share_x), F32),
            pltpu.VMEM((depth_z, share_x), F32),
            pltpu.VMEM((2, depth_y, depth_y), BF16),
            pltpu.VMEM((2, width, width), BF16),
            pltpu.VMEM((n_py, rows_y, share_x), F32),
            pltpu.VMEM((depth_y, share_x), F32),
            pltpu.VMEM((depth_y // 2, share_x), F32),
            pltpu.SemaphoreType.DMA((fields,)),
            pltpu.SemaphoreType.DMA((7,)),
            pltpu.SemaphoreType.DMA((fields,)),
            pltpu.SemaphoreType.DMA((fields,)),
            pltpu.SemaphoreType.DMA((fields,)),
            pltpu.SemaphoreType.DMA((fields + share_y * nz // width - 1,)),
            pltpu.SemaphoreType.DMA((1,)),
            pltpu.SemaphoreType.DMA((1,)),
            pltpu.SemaphoreType.DMA((n_py,)),
            pltpu.SemaphoreType.DMA((1,)),
            pltpu.SemaphoreType.DMA((1,)),
        ],
        compiler_params=pltpu.CompilerParams(
            collective_id=0, has_side_effects=True, vmem_limit_bytes=54500000
        ),
    )(
        *(
            pltpu.with_memory_space_constraint(x, pltpu.HBM)
            for x in (
                values,
                jnp.asarray(split_table(nx)),
                jnp.asarray(split_table(ny)),
                jnp.asarray(split_table(nz)),
                coupling,
                symbol_x.reshape(1, nx),
                symbol_y,
                symbol_z.reshape(1, nz),
            )
        )
    )
    return jnp.transpose(out.reshape(fields, share_y, nz, share_x), (0, 3, 1, 2))


def solution(mesh):
    return jax.shard_map(
        functools.partial(shards, mesh.shape["py"], mesh.shape["pz"]),
        mesh=mesh,
        in_specs=(P(None, None, "py", "pz"), P(), P(), P(), P()),
        out_specs=P(None, "py", "pz", None),
        check_vma=False,
    )
```

```python
import functools

import jax
import jax.numpy as jnp
import numpy as np
from jax import lax
from jax.experimental import pallas as pl
from jax.experimental.pallas import tpu as pltpu
from jax.sharding import PartitionSpec as P

MESH = pl.DeviceIdType.MESH
F32 = jnp.float32
BF16 = jnp.bfloat16
LANES, SUBLANES = 128, 8
VMEM_BUDGET = 48 << 20
RAW_SHARES = ((0, 1, 3), (0, 2))


def mode_table(count):
    rank = jnp.arange(count)
    angle = (
        jnp.pi
        / (4 * count)
        * ((2 * rank[:, None] + 1) * (2 * rank[None, :] + 1) % (8 * count)).astype(jnp.float32)
    )
    return jnp.cos(angle) * (2.0 / count) ** 0.5


def transform_dim(values, dim):
    moved = jnp.tensordot(
        values, mode_table(values.shape[dim]), axes=([dim], [0]), precision=lax.Precision.HIGHEST
    )
    return jnp.moveaxis(moved, -1, dim)


def plain_shards(species, coupling, symbol_x, symbol_y, symbol_z):
    values = transform_dim(species, 1)
    values = lax.all_to_all(values, "py", split_axis=1, concat_axis=2, tiled=True)
    values = transform_dim(values, 2)
    values = lax.all_to_all(values, "pz", split_axis=2, concat_axis=3, tiled=True)
    values = transform_dim(values, 3)
    share_x = values.shape[1]
    part_x = lax.dynamic_slice_in_dim(symbol_x, lax.axis_index("py") * share_x, share_x)
    share_y = values.shape[2]
    part_y = lax.dynamic_slice_in_dim(symbol_y, lax.axis_index("pz") * share_y, share_y)
    symbol = part_x[:, None, None] + part_y[None, :, None] + symbol_z[None, None, :]
    weight = 1.0 / (1.0 + symbol)
    mixed = jnp.einsum("ab,bxyz->axyz", coupling, values, precision=lax.Precision.HIGHEST)
    return weight * values + (1.0 - weight) * mixed


def split_table(count):
    rank = 2 * np.arange(count) + 1
    table = np.cos(np.pi / (4 * count) * (rank[:, None] * rank[None, :] % (8 * count)))
    table = (table * np.sqrt(2.0 / count)).astype(np.float32)
    high = table.astype(BF16)
    low = (table - high.astype(np.float32)).astype(BF16)
    return np.stack([high, low])


def split(values):
    high = values.astype(BF16)
    low = (values - high.astype(F32)).astype(BF16)
    return high, low


def dot(a, b):
    return jnp.dot(a, b, preferred_element_type=F32)


def flipped(index, offset, count):
    if count & (count - 1):
        return lax.rem(index + offset, count)
    result = index
    bit = 1
    while bit < count:
        if offset & bit:
            result = result + bit - 2 * bit * lax.rem(index // bit, 2)
        bit *= 2
    return result


def source_of(index, offset, count):
    if count & (count - 1):
        return lax.rem(index + count - offset, count)
    return flipped(index, offset, count)


def kernel(
    dims, field_ref, hx_hbm, hy_hbm, hz_hbm, coupling_hbm, sx_hbm, sy_hbm, sz_hbm, out_ref,
    held, hx, hy, hz, coupling, sx, sy, sz, lines_out, lines, parts_out, parts, modes, weights,
    my, mz, far, far_lines, far_out, load_sem, side_sem, send_y, recv_y, send_z, recv_z,
    send_raw, recv_raw, send_relay, recv_relay, send_far,
):
    fields, ny, nz, n_py, n_pz, yl, zl, share_x, share_y = dims
    py, pz = lax.axis_index("py"), lax.axis_index("pz")
    rows_y = yl * zl
    rows_z = share_y * zl
    depth_y = ny * zl
    group = max(g for g in range(1, share_y + 1) if share_y % g == 0 and g * nz <= max(nz, 256))
    rows_g, rows_out = group * zl, group * nz
    depth_g = n_pz * rows_g

    def load(f):
        return pltpu.make_async_copy(field_ref.at[f], held.at[f], load_sem.at[f])

    pairs = (
        (hx_hbm.at[0], hx.at[0]), (hx_hbm.at[1], hx.at[1]), (hy_hbm, hy), (hz_hbm, hz),
        (coupling_hbm, coupling), (sx_hbm, sx), (sy_hbm, sy), (sz_hbm, sz),
    )
    sides = [
        pltpu.make_async_copy(a, b, side_sem.at[i]) for i, (a, b) in enumerate(pairs)
    ]
    barrier = pltpu.get_barrier_semaphore()
    for o in range(n_pz - 1, 0, -1):
        pl.semaphore_signal(
            barrier, inc=1, device_id={"pz": flipped(pz, o, n_pz)}, device_id_type=MESH
        )
    for o in range(n_py - 1, 0, -1):
        pl.semaphore_signal(
            barrier, inc=1, device_id={"py": flipped(py, o, n_py)}, device_id_type=MESH
        )
    load(0).start()
    sides[0].start()
    sides[1].start()

    def copy_y(f, o):
        to = flipped(py, o, n_py)
        return pltpu.make_async_remote_copy(
            src_ref=lines_out.at[f, to],
            dst_ref=lines.at[f, pl.ds(py * rows_y, rows_y)],
            send_sem=send_y.at[f],
            recv_sem=recv_y.at[f],
            device_id={"py": to},
            device_id_type=MESH,
        )

    near = n_pz // 2
    half = pz // near

    def across(j):
        return (1 - half) * (n_pz - 1 - j) + half * j

    def beside(o):
        return flipped(pz, o, n_pz)

    def copy_z(f, peer, piece=None):
        rows, first = (rows_z, 0) if piece is None else (rows_g, piece * rows_g)
        return pltpu.make_async_remote_copy(
            src_ref=parts_out.at[f, pl.ds(peer * rows_z + first, rows)],
            dst_ref=parts.at[f, pl.ds(pz * rows_z + first, rows)],
            send_sem=send_z.at[f],
            recv_sem=recv_z.at[f if piece is None else f + piece],
            device_id={"pz": peer},
            device_id_type=MESH,
        )

    def wait_for(ref, sem):
        pltpu.make_async_copy(ref, ref, sem).wait()

    def wait_lines(f):
        wait_for(lines.at[f, pl.ds(0, (n_py - 1) * rows_y)], recv_y.at[f])

    mirror = flipped(pz, near, n_pz)
    early = lax.rem(pz, 2) == 0
    pair = lax.rem(pz // 2, 2)

    def is_raw(share):
        found = jnp.bool_(False)
        for bit, shares in enumerate(RAW_SHARES):
            for s in shares:
                found = found | ((pair == bit) & (share == s))
        return early & found

    raw_role = is_raw(py)
    plain_role = jnp.logical_not(raw_role)

    def each_pair(do):
        for bit, shares in enumerate(RAW_SHARES):
            pl.when(early & (pair == bit))(functools.partial(do, shares))

    def copy_raw(share):
        return pltpu.make_async_remote_copy(
            src_ref=lines_out.at[0, share],
            dst_ref=far.at[share],
            send_sem=send_raw.at[0],
            recv_sem=recv_raw.at[0],
            device_id={"pz": mirror},
            device_id_type=MESH,
        )

    def send_raws(shares):
        for share in shares:
            copy_raw(share).start()

    def copy_relay(o):
        to = flipped(py, o, n_py)
        return pltpu.make_async_remote_copy(
            src_ref=far.at[to],
            dst_ref=far_lines.at[pl.ds(py * rows_y, rows_y)],
            send_sem=send_relay.at[o],
            recv_sem=recv_relay.at[0],
            device_id={"py": to},
            device_id_type=MESH,
        )

    def copy_far(o):
        to = flipped(pz, o, n_pz)
        return pltpu.make_async_remote_copy(
            src_ref=far_out.at[pl.ds((to - half * near) * rows_z, rows_z)],
            dst_ref=parts.at[0, pl.ds(mirror * rows_z, rows_z)],
            send_sem=send_far.at[0],
            recv_sem=recv_z.at[0],
            device_id={"pz": to},
            device_id_type=MESH,
        )

    for f in range(fields):
        load(f).wait()
        high, low = split(held[f])
        if f == 0:
            sides[0].wait()
            for later in range(1, fields):
                load(later).start()
            for side in sides[2:]:
                side.start()
        both = dot(jnp.concatenate([high, low], axis=0), hx[0])
        if f == 0:
            sides[1].wait()
        result = both[:rows_y] + both[rows_y:] + dot(high, hx[1])
        for d in range(n_py):
            lines_out[f, d] = result[:, d * share_x : (d + 1) * share_x]
        def send_lines(f, when=None):
            for o in (1, 2, 3):
                start = copy_y(f, o).start
                if when is None:
                    start()
                else:
                    pl.when(is_raw(flipped(py, o, n_py)) == when)(start)

        if f == 0:
            pl.semaphore_wait(barrier, n_py + n_pz - 2)
            each_pair(send_raws)
            pl.when(jnp.logical_not(early))(functools.partial(send_lines, 0))
        elif f == 1:
            pl.when(early)(functools.partial(send_lines, 0, False))
            pl.when(jnp.logical_not(early))(functools.partial(send_lines, 1))
        else:
            if f == 2:
                pl.when(early)(functools.partial(send_lines, 1))
                send_lines(0, True)
            send_lines(f)
        lines[f, pl.ds(py * rows_y, rows_y)] = lines_out[f, py]

    for side in sides[2:]:
        side.wait()

    def iota(shape, dim):
        return lax.broadcasted_iota(jnp.int32, shape, dim)

    row, col = iota((depth_y, ny), 0), iota((depth_y, ny), 1)
    pick = (row // zl == col).astype(F32).astype(BF16)
    row, col = iota((ny, depth_y), 0), iota((ny, depth_y), 1)
    spread = (col // zl == row).astype(F32).astype(BF16)
    row, col = iota((depth_y, depth_y), 0), iota((depth_y, depth_y), 1)
    keep = row % zl == col % zl
    for t in range(2):
        wide = dot(dot(pick, hy[t]).astype(BF16), spread)
        my[t] = jnp.where(keep, wide, 0.0).astype(BF16)
    def rows_transform(high_table, low_table, high, low):
        both = dot(high_table, jnp.concatenate([high, low], axis=1))
        return both[:, :share_x] + both[:, share_x:] + dot(low_table, high)

    half_rows = depth_y // 2

    last = fields - 1
    pieces = share_y // group

    def send_parts(f, peers):
        for piece in range(pieces) if f == last else [None]:
            for peer in peers:
                copy_z(f, peer, piece).start()

    deep = lax.rem(pz // (near // 2), 2) == half
    outer = [across(j) for j in range(near // 2)]
    inner = [across(j) for j in range(near // 2, near)]
    around = [beside(o) for o in range(near - 1, 0, -1)]

    def y_step(f, before):
        wait_lines(f)
        high, low = split(lines[f])
        def transform(first, rows):
            span = pl.ds(pl.multiple_of(first, rows), rows)
            parts_out[f, span] = rows_transform(my[0, span], my[1, span], high, low)

        quarter = half_rows // 2
        far_half = (1 - half) * half_rows
        transform(far_half + (1 - half) * quarter, quarter)
        send_parts(f, outer)
        transform(far_half + half * quarter, quarter)
        if before is not None:
            pl.when(jnp.logical_not(deep))(functools.partial(send_parts, before, inner))
        if f == last:
            send_parts(f, inner)
        else:
            pl.when(deep)(functools.partial(send_parts, f, inner))
        transform(half * half_rows, half_rows)
        send_parts(f, around)
        parts[f, pl.ds(pz * rows_z, rows_z)] = parts_out[f, pl.ds(pz * rows_z, rows_z)]

    def relay():
        each_pair(lambda shares: wait_for(far.at[pl.ds(0, len(shares))], recv_raw.at[0]))
        for o in range(n_py - 1, 0, -1):
            pl.when(is_raw(flipped(py, o, n_py)))(copy_relay(o).start)

        @pl.when(raw_role)
        def _():
            far_lines[pl.ds(py * rows_y, rows_y)] = far[py]

    def near_step():
        wait_lines(0)
        span = pl.ds(pl.multiple_of(half * half_rows, half_rows), half_rows)
        high, low = split(lines[0])
        parts_out[0, span] = rows_transform(my[0, span], my[1, span], high, low)
        send_parts(0, around)
        parts[0, pl.ds(pz * rows_z, rows_z)] = parts_out[0, pl.ds(pz * rows_z, rows_z)]
        wait_for(far_lines.at[pl.ds(0, (n_py - 1) * rows_y)], recv_relay.at[0])
        high, low = split(far_lines[...])
        far_out[...] = rows_transform(my[0, span], my[1, span], high, low)
        for o in range(near - 1, 0, -1):
            copy_far(o).start()
        parts[0, pl.ds(mirror * rows_z, rows_z)] = far_out[
            pl.ds((pz - half * near) * rows_z, rows_z)
        ]

    pl.when(plain_role)(functools.partial(y_step, 0, None))
    for f in range(1, fields):
        if f == fields - 1:
            pl.when(raw_role)(near_step)
        if f == 1:
            pl.when(plain_role & jnp.logical_not(deep))(functools.partial(send_parts, 0, inner))
        y_step(f, f - 1 if f > 1 else None)
        if f == 1:
            relay()

    row, col = iota((rows_out, nz), 0), iota((rows_out, nz), 1)
    pick = (row % nz == col).astype(F32).astype(BF16)
    row, col = iota((nz, depth_g), 0), iota((nz, depth_g), 1)
    spread = ((col // rows_g) * zl + col % zl == row).astype(F32).astype(BF16)
    row, col = iota((rows_out, depth_g), 0), iota((rows_out, depth_g), 1)
    keep = row // nz == (col // zl) % group
    for t in range(2):
        wide = dot(dot(pick, hz[t]).astype(BF16), spread)
        mz[t] = jnp.where(keep, wide, 0.0).astype(BF16)

    def z_step(f, g):
        starts = [p * rows_z + g * rows_g for p in range(n_pz)]
        block = jnp.concatenate([parts[f, a : a + rows_g] for a in starts], axis=0)
        return rows_transform(mz[0], mz[1], *split(block))

    diagonal = iota((nz, nz), 0) == iota((nz, nz), 1)
    sz_column = jnp.sum(jnp.where(diagonal, sz[...], 0.0), axis=1, keepdims=True)
    sx_row = sx[:, pl.ds(pl.multiple_of(py * share_x, share_x), share_x)]
    for k in range(share_y):
        symbol = (sx_row + sy[pz * share_y + k]) + sz_column
        weights[pl.ds(k * nz, nz)] = 1.0 / (1.0 + symbol)

    def wait_parts(f, blocks):
        wait_for(parts.at[f, pl.ds(0, blocks * rows_z)], recv_z.at[f])

    for f in [*range(1, last), 0, last]:
        if f == 0:
            pl.when(raw_role)(functools.partial(wait_parts, 0, n_pz - 2))
            pl.when(plain_role)(functools.partial(wait_parts, 0, n_pz - 1))
        elif f < last:
            wait_parts(f, n_pz - 1)
        if f < last:
            for g in range(pieces):
                modes[f, pl.ds(g * rows_out, rows_out)] = z_step(f, g)
        if f == 0:
            for k in range(share_y):
                span = pl.ds(k * nz, nz)
                weight = weights[span]
                old = [modes[b, span] for b in range(last)]
                for a in range(fields):
                    mixed = coupling[a, 0] * old[0]
                    for b in range(1, last):
                        mixed = mixed + coupling[a, b] * old[b]
                    mixed = (1.0 - weight) * mixed
                    out_ref[a, span] = mixed + weight * old[a] if a < last else mixed
        if f == last:
            for g in range(pieces):
                wait_for(parts.at[f, pl.ds(0, (n_pz - 1) * rows_g)], recv_z.at[f + g])
                span = pl.ds(g * rows_out, rows_out)
                result = z_step(f, g)
                weight = weights[span]
                rest = (1.0 - weight) * result
                for a in range(fields):
                    new = out_ref[a, span] + coupling[a, last] * rest
                    out_ref[a, span] = new + weight * result if a == last else new
    def sent_parts(f, blocks):
        wait_for(parts_out.at[f, pl.ds(0, blocks * rows_z)], send_z.at[f])

    for f in range(fields):
        wait_for(lines_out.at[f, pl.ds(0, n_py - 1)], send_y.at[f])
        if f:
            sent_parts(f, n_pz - 1)

    each_pair(lambda shares: wait_for(far.at[pl.ds(0, len(shares))], send_raw.at[0]))
    for o in range(1, n_py):
        pl.when(is_raw(flipped(py, o, n_py)))(copy_relay(o).wait_send)

    @pl.when(raw_role)
    def _():
        wait_for(far_out.at[pl.ds(0, (near - 1) * rows_z)], send_far.at[0])
        sent_parts(0, near - 1)

    @pl.when(plain_role)
    def _():
        sent_parts(0, n_pz - 1)


def shards(n_py, n_pz, species, coupling, symbol_x, symbol_y, symbol_z):
    fields, nx, yl, zl = species.shape
    ny, nz = yl * n_py, zl * n_pz
    share_x, share_y = nx // n_py, ny // n_pz
    block = fields * nx * yl * zl
    tables = 2 * (nx * nx + (ny * zl) ** 2 + (share_y * nz) ** 2)
    need = 7 * 4 * block + 2 * tables + 16 * max(ny * zl, share_y * nz) ** 2
    bad = share_x % LANES or zl % SUBLANES or nx % n_py or ny % n_pz
    if bad or need > VMEM_BUDGET or fields < 3 or n_pz % 4 or n_pz & (n_pz - 1):
        return plain_shards(species, coupling, symbol_x, symbol_y, symbol_z)
    dims = (fields, ny, nz, n_py, n_pz, yl, zl, share_x, share_y)
    rows_y, depth_y, depth_z = yl * zl, ny * zl, share_y * nz
    width = nz * max(g for g in range(1, share_y + 1) if share_y % g == 0 and g * nz <= max(nz, 256))
    vmem = pl.BlockSpec(memory_space=pltpu.VMEM)
    hbm = pl.BlockSpec(memory_space=pltpu.HBM)
    values = jnp.transpose(species, (0, 2, 3, 1)).reshape(fields, rows_y, nx)
    out = pl.pallas_call(
        functools.partial(kernel, dims),
        out_shape=jax.ShapeDtypeStruct((fields, depth_z, share_x), F32),
        in_specs=[hbm] * 8,
        out_specs=vmem,
        scratch_shapes=[
            pltpu.VMEM((fields, rows_y, nx), F32),
            pltpu.VMEM((2, nx, nx), BF16),
            pltpu.VMEM((2, ny, ny), BF16),
            pltpu.VMEM((2, nz, nz), BF16),
            pltpu.SMEM((fields, fields), F32),
            pltpu.VMEM((1, nx), F32),
            pltpu.SMEM((ny,), F32),
            pltpu.VMEM((1, nz), F32),
            pltpu.VMEM((fields, n_py, rows_y, share_x), F32),
            pltpu.VMEM((fields, depth_y, share_x), F32),
            pltpu.VMEM((fields, depth_y, share_x), F32),
            pltpu.VMEM((fields, depth_z, share_x), F32),
            pltpu.VMEM((fields - 1, depth_z, share_x), F32),
            pltpu.VMEM((depth_z, share_x), F32),
            pltpu.VMEM((2, depth_y, depth_y), BF16),
            pltpu.VMEM((2, width, width), BF16),
            pltpu.VMEM((n_py, rows_y, share_x), F32),
            pltpu.VMEM((depth_y, share_x), F32),
            pltpu.VMEM((depth_y // 2, share_x), F32),
            pltpu.SemaphoreType.DMA((fields,)),
            pltpu.SemaphoreType.DMA((8,)),
            pltpu.SemaphoreType.DMA((fields,)),
            pltpu.SemaphoreType.DMA((fields,)),
            pltpu.SemaphoreType.DMA((fields,)),
            pltpu.SemaphoreType.DMA((fields + share_y * nz // width - 1,)),
            pltpu.SemaphoreType.DMA((1,)),
            pltpu.SemaphoreType.DMA((1,)),
            pltpu.SemaphoreType.DMA((n_py,)),
            pltpu.SemaphoreType.DMA((1,)),
            pltpu.SemaphoreType.DMA((1,)),
        ],
        compiler_params=pltpu.CompilerParams(
            collective_id=0, has_side_effects=True, vmem_limit_bytes=54500000
        ),
    )(
        *(
            pltpu.with_memory_space_constraint(x, pltpu.HBM)
            for x in (
                values,
                jnp.asarray(split_table(nx)),
                jnp.asarray(split_table(ny)),
                jnp.asarray(split_table(nz)),
                coupling,
                symbol_x.reshape(1, nx),
                symbol_y,
                symbol_z.reshape(1, nz),
            )
        )
    )
    return jnp.transpose(out.reshape(fields, share_y, nz, share_x), (0, 3, 1, 2))


def solution(mesh):
    return jax.shard_map(
        functools.partial(shards, mesh.shape["py"], mesh.shape["pz"]),
        mesh=mesh,
        in_specs=(P(None, None, "py", "pz"), P(), P(), P(), P()),
        out_specs=P(None, "py", "pz", None),
        check_vma=False,
    )
```

```python
import functools

import jax
import jax.numpy as jnp
import numpy as np
from jax import lax
from jax.experimental import pallas as pl
from jax.experimental.pallas import tpu as pltpu
from jax.sharding import PartitionSpec as P

MESH = pl.DeviceIdType.MESH
F32 = jnp.float32
BF16 = jnp.bfloat16
LANES, SUBLANES = 128, 8
VMEM_BUDGET = 48 << 20


def mode_table(count):
    rank = jnp.arange(count)
    angle = (
        jnp.pi
        / (4 * count)
        * ((2 * rank[:, None] + 1) * (2 * rank[None, :] + 1) % (8 * count)).astype(jnp.float32)
    )
    return jnp.cos(angle) * (2.0 / count) ** 0.5


def transform_dim(values, dim):
    moved = jnp.tensordot(
        values, mode_table(values.shape[dim]), axes=([dim], [0]), precision=lax.Precision.HIGHEST
    )
    return jnp.moveaxis(moved, -1, dim)


def plain_shards(species, coupling, symbol_x, symbol_y, symbol_z):
    values = transform_dim(species, 1)
    values = lax.all_to_all(values, "py", split_axis=1, concat_axis=2, tiled=True)
    values = transform_dim(values, 2)
    values = lax.all_to_all(values, "pz", split_axis=2, concat_axis=3, tiled=True)
    values = transform_dim(values, 3)
    share_x = values.shape[1]
    part_x = lax.dynamic_slice_in_dim(symbol_x, lax.axis_index("py") * share_x, share_x)
    share_y = values.shape[2]
    part_y = lax.dynamic_slice_in_dim(symbol_y, lax.axis_index("pz") * share_y, share_y)
    symbol = part_x[:, None, None] + part_y[None, :, None] + symbol_z[None, None, :]
    weight = 1.0 / (1.0 + symbol)
    mixed = jnp.einsum("ab,bxyz->axyz", coupling, values, precision=lax.Precision.HIGHEST)
    return weight * values + (1.0 - weight) * mixed


def split_table(count):
    rank = 2 * np.arange(count) + 1
    table = np.cos(np.pi / (4 * count) * (rank[:, None] * rank[None, :] % (8 * count)))
    table = (table * np.sqrt(2.0 / count)).astype(np.float32)
    high = table.astype(BF16)
    low = (table - high.astype(np.float32)).astype(BF16)
    return np.stack([high, low])


def split(values):
    high = values.astype(BF16)
    low = (values - high.astype(F32)).astype(BF16)
    return high, low


def dot(a, b):
    return jnp.dot(a, b, preferred_element_type=F32)


def flipped(index, offset, count):
    if count & (count - 1):
        return lax.rem(index + offset, count)
    result = index
    bit = 1
    while bit < count:
        if offset & bit:
            result = result + bit - 2 * bit * lax.rem(index // bit, 2)
        bit *= 2
    return result


def source_of(index, offset, count):
    if count & (count - 1):
        return lax.rem(index + count - offset, count)
    return flipped(index, offset, count)


def kernel(
    dims, field_ref, hx_hbm, hy_hbm, hz_hbm, coupling_hbm, sx_hbm, sy_hbm, sz_hbm, out_ref,
    held, hx, hy, hz, coupling, sx, sy, sz, lines_out, lines, parts_out, parts, modes, weights,
    my, mz, far, far_lines, far_out, load_sem, side_sem, send_y, recv_y, send_z, recv_z,
    send_raw, recv_raw, send_relay, recv_relay, send_far,
):
    fields, ny, nz, n_py, n_pz, yl, zl, share_x, share_y = dims
    py, pz = lax.axis_index("py"), lax.axis_index("pz")
    rows_y = yl * zl
    rows_z = share_y * zl
    depth_y = ny * zl
    group = max(g for g in range(1, share_y + 1) if share_y % g == 0 and g * nz <= max(nz, 256))
    rows_g, rows_out = group * zl, group * nz
    depth_g = n_pz * rows_g

    def load(f):
        return pltpu.make_async_copy(field_ref.at[f], held.at[f], load_sem.at[f])

    pairs = (
        (hx_hbm.at[0], hx.at[0]), (hx_hbm.at[1], hx.at[1]), (hy_hbm, hy), (hz_hbm, hz),
        (coupling_hbm, coupling), (sx_hbm, sx), (sy_hbm, sy), (sz_hbm, sz),
    )
    sides = [
        pltpu.make_async_copy(a, b, side_sem.at[i]) for i, (a, b) in enumerate(pairs)
    ]
    barrier = pltpu.get_barrier_semaphore()
    for o in range(n_pz - 1, 0, -1):
        pl.semaphore_signal(
            barrier, inc=1, device_id={"pz": flipped(pz, o, n_pz)}, device_id_type=MESH
        )
    for o in range(n_py - 1, 0, -1):
        pl.semaphore_signal(
            barrier, inc=1, device_id={"py": flipped(py, o, n_py)}, device_id_type=MESH
        )
    load(0).start()
    sides[0].start()
    sides[1].start()

    def copy_y(f, o):
        to = flipped(py, o, n_py)
        return pltpu.make_async_remote_copy(
            src_ref=lines_out.at[f, to],
            dst_ref=lines.at[f, pl.ds(py * rows_y, rows_y)],
            send_sem=send_y.at[f],
            recv_sem=recv_y.at[f],
            device_id={"py": to},
            device_id_type=MESH,
        )

    near = n_pz // 2
    half = pz // near

    def across(j):
        return (1 - half) * (n_pz - 1 - j) + half * j

    def beside(o):
        return flipped(pz, o, n_pz)

    def copy_z(f, peer, piece=None):
        rows, first = (rows_z, 0) if piece is None else (rows_g, piece * rows_g)
        return pltpu.make_async_remote_copy(
            src_ref=parts_out.at[f, pl.ds(peer * rows_z + first, rows)],
            dst_ref=parts.at[f, pl.ds(pz * rows_z + first, rows)],
            send_sem=send_z.at[f],
            recv_sem=recv_z.at[f if piece is None else f + piece],
            device_id={"pz": peer},
            device_id_type=MESH,
        )

    def wait_for(ref, sem):
        pltpu.make_async_copy(ref, ref, sem).wait()

    def wait_lines(f):
        wait_for(lines.at[f, pl.ds(0, (n_py - 1) * rows_y)], recv_y.at[f])

    mirror = flipped(pz, near, n_pz)
    early = lax.rem(pz, 2) == 0
    pair = lax.rem(pz // 2, 2)

    raw_shares = (tuple(range(0, n_py, 2)), (0, *range(1, n_py, 2)))

    def is_raw(share):
        found = jnp.bool_(False)
        for bit, shares in enumerate(raw_shares):
            for s in shares:
                found = found | ((pair == bit) & (share == s))
        return early & found

    raw_role = is_raw(py)
    plain_role = jnp.logical_not(raw_role)

    def each_pair(do):
        for bit, shares in enumerate(raw_shares):
            pl.when(early & (pair == bit))(functools.partial(do, shares))

    def copy_raw(share):
        return pltpu.make_async_remote_copy(
            src_ref=lines_out.at[0, share],
            dst_ref=far.at[share],
            send_sem=send_raw.at[0],
            recv_sem=recv_raw.at[0],
            device_id={"pz": mirror},
            device_id_type=MESH,
        )

    def send_raws(shares):
        for share in shares:
            copy_raw(share).start()

    def copy_relay(o):
        to = flipped(py, o, n_py)
        return pltpu.make_async_remote_copy(
            src_ref=far.at[to],
            dst_ref=far_lines.at[pl.ds(py * rows_y, rows_y)],
            send_sem=send_relay.at[o],
            recv_sem=recv_relay.at[0],
            device_id={"py": to},
            device_id_type=MESH,
        )

    def copy_far(o):
        to = flipped(pz, o, n_pz)
        return pltpu.make_async_remote_copy(
            src_ref=far_out.at[pl.ds((to - half * near) * rows_z, rows_z)],
            dst_ref=parts.at[0, pl.ds(mirror * rows_z, rows_z)],
            send_sem=send_far.at[0],
            recv_sem=recv_z.at[0],
            device_id={"pz": to},
            device_id_type=MESH,
        )

    last = fields - 1
    late_role = jnp.logical_not(early)

    def send_lines(f, when=None):
        for o in range(1, n_py):
            start = copy_y(f, o).start
            if when is None:
                start()
            else:
                pl.when(is_raw(flipped(py, o, n_py)) == when)(start)

    for f in range(fields):
        load(f).wait()
        high, low = split(held[f])
        if f == 0:
            sides[0].wait()
            for later in range(1, fields):
                load(later).start()
            for side in sides[2:]:
                side.start()
        both = dot(jnp.concatenate([high, low], axis=0), hx[0])
        if f == 0:
            sides[1].wait()
        result = both[:rows_y] + both[rows_y:] + dot(high, hx[1])
        for d in range(n_py):
            lines_out[f, d] = result[:, d * share_x : (d + 1) * share_x]
        if f == 0:
            pl.semaphore_wait(barrier, n_py + n_pz - 2)
            each_pair(send_raws)
            pl.when(late_role)(functools.partial(send_lines, 0))
        elif f < last:
            if f == 1:
                pl.when(early)(functools.partial(send_lines, 0, False))
            pl.when(late_role)(functools.partial(send_lines, f))
        else:
            for held_back in range(1, last):
                pl.when(early)(functools.partial(send_lines, held_back))
            send_lines(0, True)
            send_lines(last)
        lines[f, pl.ds(py * rows_y, rows_y)] = lines_out[f, py]

    for side in sides[2:]:
        side.wait()

    def iota(shape, dim):
        return lax.broadcasted_iota(jnp.int32, shape, dim)

    row, col = iota((depth_y, ny), 0), iota((depth_y, ny), 1)
    pick = (row // zl == col).astype(F32).astype(BF16)
    row, col = iota((ny, depth_y), 0), iota((ny, depth_y), 1)
    spread = (col // zl == row).astype(F32).astype(BF16)
    row, col = iota((depth_y, depth_y), 0), iota((depth_y, depth_y), 1)
    keep = row % zl == col % zl
    for t in range(2):
        wide = dot(dot(pick, hy[t]).astype(BF16), spread)
        my[t] = jnp.where(keep, wide, 0.0).astype(BF16)
    def rows_transform(high_table, low_table, high, low):
        both = dot(high_table, jnp.concatenate([high, low], axis=1))
        return both[:, :share_x] + both[:, share_x:] + dot(low_table, high)

    half_rows = depth_y // 2

    pieces = share_y // group

    def send_parts(f, peers):
        for piece in range(pieces) if f == last else [None]:
            for peer in peers:
                copy_z(f, peer, piece).start()

    deep = lax.rem(pz // (near // 2), 2) == half
    outer = [across(j) for j in range(near // 2)]
    inner = [across(j) for j in range(near // 2, near)]
    around = [beside(o) for o in range(near - 1, 0, -1)]

    def y_step(f, before):
        wait_lines(f)
        high, low = split(lines[f])
        def transform(first, rows):
            span = pl.ds(pl.multiple_of(first, rows), rows)
            parts_out[f, span] = rows_transform(my[0, span], my[1, span], high, low)

        quarter = half_rows // 2
        far_half = (1 - half) * half_rows
        transform(far_half + (1 - half) * quarter, quarter)
        send_parts(f, outer)
        transform(far_half + half * quarter, quarter)
        if before is not None:
            pl.when(jnp.logical_not(deep))(functools.partial(send_parts, before, inner))
        if f == last:
            send_parts(f, inner)
        else:
            pl.when(deep)(functools.partial(send_parts, f, inner))
        transform(half * half_rows, half_rows)
        send_parts(f, around)
        parts[f, pl.ds(pz * rows_z, rows_z)] = parts_out[f, pl.ds(pz * rows_z, rows_z)]

    def relay():
        each_pair(lambda shares: wait_for(far.at[pl.ds(0, len(shares))], recv_raw.at[0]))
        for o in range(n_py - 1, 0, -1):
            pl.when(is_raw(flipped(py, o, n_py)))(copy_relay(o).start)

        @pl.when(raw_role)
        def _():
            far_lines[pl.ds(py * rows_y, rows_y)] = far[py]

    def near_step():
        wait_lines(0)
        span = pl.ds(pl.multiple_of(half * half_rows, half_rows), half_rows)
        high, low = split(lines[0])
        parts_out[0, span] = rows_transform(my[0, span], my[1, span], high, low)
        send_parts(0, around)
        parts[0, pl.ds(pz * rows_z, rows_z)] = parts_out[0, pl.ds(pz * rows_z, rows_z)]
        wait_for(far_lines.at[pl.ds(0, (n_py - 1) * rows_y)], recv_relay.at[0])
        high, low = split(far_lines[...])
        far_out[...] = rows_transform(my[0, span], my[1, span], high, low)
        for o in range(near - 1, 0, -1):
            copy_far(o).start()
        parts[0, pl.ds(mirror * rows_z, rows_z)] = far_out[
            pl.ds((pz - half * near) * rows_z, rows_z)
        ]

    pl.when(plain_role)(functools.partial(y_step, 0, None))
    for f in range(1, fields):
        if f == fields - 1:
            pl.when(raw_role)(near_step)
        if f == 1:
            pl.when(plain_role & jnp.logical_not(deep))(functools.partial(send_parts, 0, inner))
        y_step(f, f - 1 if f > 1 else None)
        if f == 1:
            relay()

    row, col = iota((rows_out, nz), 0), iota((rows_out, nz), 1)
    pick = (row % nz == col).astype(F32).astype(BF16)
    row, col = iota((nz, depth_g), 0), iota((nz, depth_g), 1)
    spread = ((col // rows_g) * zl + col % zl == row).astype(F32).astype(BF16)
    row, col = iota((rows_out, depth_g), 0), iota((rows_out, depth_g), 1)
    keep = row // nz == (col // zl) % group
    for t in range(2):
        wide = dot(dot(pick, hz[t]).astype(BF16), spread)
        mz[t] = jnp.where(keep, wide, 0.0).astype(BF16)

    def z_step(f, g):
        starts = [p * rows_z + g * rows_g for p in range(n_pz)]
        block = jnp.concatenate([parts[f, a : a + rows_g] for a in starts], axis=0)
        return rows_transform(mz[0], mz[1], *split(block))

    diagonal = iota((nz, nz), 0) == iota((nz, nz), 1)
    sz_column = jnp.sum(jnp.where(diagonal, sz[...], 0.0), axis=1, keepdims=True)
    sx_row = sx[:, pl.ds(pl.multiple_of(py * share_x, share_x), share_x)]
    for k in range(share_y):
        symbol = (sx_row + sy[pz * share_y + k]) + sz_column
        weights[pl.ds(k * nz, nz)] = 1.0 / (1.0 + symbol)

    def wait_parts(f, blocks):
        wait_for(parts.at[f, pl.ds(0, blocks * rows_z)], recv_z.at[f])

    for f in [*range(1, last), 0, last]:
        if f == 0:
            pl.when(raw_role)(functools.partial(wait_parts, 0, n_pz - 2))
            pl.when(plain_role)(functools.partial(wait_parts, 0, n_pz - 1))
        elif f < last:
            wait_parts(f, n_pz - 1)
        if f < last:
            for g in range(pieces):
                modes[f, pl.ds(g * rows_out, rows_out)] = z_step(f, g)
        if f == 0:
            for k in range(share_y):
                span = pl.ds(k * nz, nz)
                weight = weights[span]
                old = [modes[b, span] for b in range(last)]
                for a in range(fields):
                    mixed = coupling[a, 0] * old[0]
                    for b in range(1, last):
                        mixed = mixed + coupling[a, b] * old[b]
                    mixed = (1.0 - weight) * mixed
                    out_ref[a, span] = mixed + weight * old[a] if a < last else mixed
        if f == last:
            for g in range(pieces):
                wait_for(parts.at[f, pl.ds(0, (n_pz - 1) * rows_g)], recv_z.at[f + g])
                span = pl.ds(g * rows_out, rows_out)
                result = z_step(f, g)
                weight = weights[span]
                rest = (1.0 - weight) * result
                for a in range(fields):
                    new = out_ref[a, span] + coupling[a, last] * rest
                    out_ref[a, span] = new + weight * result if a == last else new
    def sent_parts(f, blocks):
        wait_for(parts_out.at[f, pl.ds(0, blocks * rows_z)], send_z.at[f])

    for f in range(fields):
        wait_for(lines_out.at[f, pl.ds(0, n_py - 1)], send_y.at[f])
        if f:
            sent_parts(f, n_pz - 1)

    each_pair(lambda shares: wait_for(far.at[pl.ds(0, len(shares))], send_raw.at[0]))
    for o in range(1, n_py):
        pl.when(is_raw(flipped(py, o, n_py)))(copy_relay(o).wait_send)

    @pl.when(raw_role)
    def _():
        wait_for(far_out.at[pl.ds(0, (near - 1) * rows_z)], send_far.at[0])
        sent_parts(0, near - 1)

    @pl.when(plain_role)
    def _():
        sent_parts(0, n_pz - 1)


def shards(n_py, n_pz, species, coupling, symbol_x, symbol_y, symbol_z):
    fields, nx, yl, zl = species.shape
    ny, nz = yl * n_py, zl * n_pz
    share_x, share_y = nx // n_py, ny // n_pz
    block = fields * nx * yl * zl
    tables = 2 * (nx * nx + (ny * zl) ** 2 + (share_y * nz) ** 2)
    need = 7 * 4 * block + 2 * tables + 16 * max(ny * zl, share_y * nz) ** 2
    bad = share_x % LANES or zl % SUBLANES or nx % n_py or ny % n_pz
    if bad or need > VMEM_BUDGET or fields < 3 or n_pz % 4 or n_pz & (n_pz - 1):
        return plain_shards(species, coupling, symbol_x, symbol_y, symbol_z)
    dims = (fields, ny, nz, n_py, n_pz, yl, zl, share_x, share_y)
    rows_y, depth_y, depth_z = yl * zl, ny * zl, share_y * nz
    width = nz * max(g for g in range(1, share_y + 1) if share_y % g == 0 and g * nz <= max(nz, 256))
    vmem = pl.BlockSpec(memory_space=pltpu.VMEM)
    hbm = pl.BlockSpec(memory_space=pltpu.HBM)
    values = jnp.transpose(species, (0, 2, 3, 1)).reshape(fields, rows_y, nx)
    out = pl.pallas_call(
        functools.partial(kernel, dims),
        out_shape=jax.ShapeDtypeStruct((fields, depth_z, share_x), F32),
        in_specs=[hbm] * 8,
        out_specs=vmem,
        scratch_shapes=[
            pltpu.VMEM((fields, rows_y, nx), F32),
            pltpu.VMEM((2, nx, nx), BF16),
            pltpu.VMEM((2, ny, ny), BF16),
            pltpu.VMEM((2, nz, nz), BF16),
            pltpu.SMEM((fields, fields), F32),
            pltpu.VMEM((1, nx), F32),
            pltpu.SMEM((ny,), F32),
            pltpu.VMEM((1, nz), F32),
            pltpu.VMEM((fields, n_py, rows_y, share_x), F32),
            pltpu.VMEM((fields, depth_y, share_x), F32),
            pltpu.VMEM((fields, depth_y, share_x), F32),
            pltpu.VMEM((fields, depth_z, share_x), F32),
            pltpu.VMEM((fields - 1, depth_z, share_x), F32),
            pltpu.VMEM((depth_z, share_x), F32),
            pltpu.VMEM((2, depth_y, depth_y), BF16),
            pltpu.VMEM((2, width, width), BF16),
            pltpu.VMEM((n_py, rows_y, share_x), F32),
            pltpu.VMEM((depth_y, share_x), F32),
            pltpu.VMEM((depth_y // 2, share_x), F32),
            pltpu.SemaphoreType.DMA((fields,)),
            pltpu.SemaphoreType.DMA((8,)),
            pltpu.SemaphoreType.DMA((fields,)),
            pltpu.SemaphoreType.DMA((fields,)),
            pltpu.SemaphoreType.DMA((fields,)),
            pltpu.SemaphoreType.DMA((fields + share_y * nz // width - 1,)),
            pltpu.SemaphoreType.DMA((1,)),
            pltpu.SemaphoreType.DMA((1,)),
            pltpu.SemaphoreType.DMA((n_py,)),
            pltpu.SemaphoreType.DMA((1,)),
            pltpu.SemaphoreType.DMA((1,)),
        ],
        compiler_params=pltpu.CompilerParams(
            collective_id=0, has_side_effects=True, vmem_limit_bytes=54500000
        ),
    )(
        *(
            pltpu.with_memory_space_constraint(x, pltpu.HBM)
            for x in (
                values,
                jnp.asarray(split_table(nx)),
                jnp.asarray(split_table(ny)),
                jnp.asarray(split_table(nz)),
                coupling,
                symbol_x.reshape(1, nx),
                symbol_y,
                symbol_z.reshape(1, nz),
            )
        )
    )
    return jnp.transpose(out.reshape(fields, share_y, nz, share_x), (0, 3, 1, 2))


def solution(mesh):
    return jax.shard_map(
        functools.partial(shards, mesh.shape["py"], mesh.shape["pz"]),
        mesh=mesh,
        in_specs=(P(None, None, "py", "pz"), P(), P(), P(), P()),
        out_specs=P(None, "py", "pz", None),
        check_vma=False,
    )
```

```python
import functools

import jax
import jax.numpy as jnp
import numpy as np
from jax import lax
from jax.experimental import pallas as pl
from jax.experimental.pallas import tpu as pltpu
from jax.sharding import PartitionSpec as P

MESH = pl.DeviceIdType.MESH
F32 = jnp.float32
BF16 = jnp.bfloat16
LANES, SUBLANES = 128, 8
VMEM_BUDGET = 48 << 20


def mode_table(count):
    rank = jnp.arange(count)
    angle = (
        jnp.pi
        / (4 * count)
        * ((2 * rank[:, None] + 1) * (2 * rank[None, :] + 1) % (8 * count)).astype(jnp.float32)
    )
    return jnp.cos(angle) * (2.0 / count) ** 0.5


def transform_dim(values, dim):
    moved = jnp.tensordot(
        values, mode_table(values.shape[dim]), axes=([dim], [0]), precision=lax.Precision.HIGHEST
    )
    return jnp.moveaxis(moved, -1, dim)


def plain_shards(species, coupling, symbol_x, symbol_y, symbol_z):
    values = transform_dim(species, 1)
    values = lax.all_to_all(values, "py", split_axis=1, concat_axis=2, tiled=True)
    values = transform_dim(values, 2)
    values = lax.all_to_all(values, "pz", split_axis=2, concat_axis=3, tiled=True)
    values = transform_dim(values, 3)
    share_x = values.shape[1]
    part_x = lax.dynamic_slice_in_dim(symbol_x, lax.axis_index("py") * share_x, share_x)
    share_y = values.shape[2]
    part_y = lax.dynamic_slice_in_dim(symbol_y, lax.axis_index("pz") * share_y, share_y)
    symbol = part_x[:, None, None] + part_y[None, :, None] + symbol_z[None, None, :]
    weight = 1.0 / (1.0 + symbol)
    mixed = jnp.einsum("ab,bxyz->axyz", coupling, values, precision=lax.Precision.HIGHEST)
    return weight * values + (1.0 - weight) * mixed


def split_table(count):
    rank = 2 * np.arange(count) + 1
    table = np.cos(np.pi / (4 * count) * (rank[:, None] * rank[None, :] % (8 * count)))
    table = (table * np.sqrt(2.0 / count)).astype(np.float32)
    high = table.astype(BF16)
    low = (table - high.astype(np.float32)).astype(BF16)
    return np.stack([high, low])


def split(values):
    high = values.astype(BF16)
    low = (values - high.astype(F32)).astype(BF16)
    return high, low


def dot(a, b):
    return jnp.dot(a, b, preferred_element_type=F32)


def flipped(index, offset, count):
    if count & (count - 1):
        return lax.rem(index + offset, count)
    result = index
    bit = 1
    while bit < count:
        if offset & bit:
            result = result + bit - 2 * bit * lax.rem(index // bit, 2)
        bit *= 2
    return result


def source_of(index, offset, count):
    if count & (count - 1):
        return lax.rem(index + count - offset, count)
    return flipped(index, offset, count)


def kernel(
    dims, field_ref, hx_hbm, hy_hbm, hz_hbm, coupling_hbm, sx_hbm, sy_hbm, sz_hbm, out_ref,
    held, hx, hy, hz, coupling, sx, sy, sz, lines_out, lines, parts_out, parts, modes, weights,
    my, mz, far, far_lines, far_out, load_sem, side_sem, send_y, recv_y, send_z, recv_z,
    send_raw, recv_raw, send_relay, recv_relay, send_far,
):
    fields, ny, nz, n_py, n_pz, yl, zl, share_x, share_y = dims
    py, pz = lax.axis_index("py"), lax.axis_index("pz")
    rows_y = yl * zl
    rows_z = share_y * zl
    depth_y = ny * zl
    group = max(g for g in range(1, share_y + 1) if share_y % g == 0 and g * nz <= max(nz, 256))
    rows_g, rows_out = group * zl, group * nz
    depth_g = n_pz * rows_g

    def load(f):
        return pltpu.make_async_copy(field_ref.at[f], held.at[f], load_sem.at[f])

    pairs = (
        (hx_hbm.at[0], hx.at[0]), (hx_hbm.at[1], hx.at[1]), (hy_hbm, hy), (hz_hbm, hz),
        (coupling_hbm, coupling), (sx_hbm, sx), (sy_hbm, sy), (sz_hbm, sz),
    )
    sides = [
        pltpu.make_async_copy(a, b, side_sem.at[i]) for i, (a, b) in enumerate(pairs)
    ]
    barrier = pltpu.get_barrier_semaphore()
    for o in range(n_pz - 1, 0, -1):
        pl.semaphore_signal(
            barrier, inc=1, device_id={"pz": flipped(pz, o, n_pz)}, device_id_type=MESH
        )
    for o in range(n_py - 1, 0, -1):
        pl.semaphore_signal(
            barrier, inc=1, device_id={"py": flipped(py, o, n_py)}, device_id_type=MESH
        )
    load(0).start()
    sides[0].start()
    sides[1].start()

    def copy_y(f, o):
        to = flipped(py, o, n_py)
        return pltpu.make_async_remote_copy(
            src_ref=lines_out.at[f, to],
            dst_ref=lines.at[f, pl.ds(py * rows_y, rows_y)],
            send_sem=send_y.at[f],
            recv_sem=recv_y.at[fields if f == 0 and o == n_py - 1 else f],
            device_id={"py": to},
            device_id_type=MESH,
        )

    near = n_pz // 2
    half = pz // near

    def across(j):
        return (1 - half) * (n_pz - 1 - j) + half * j

    def beside(o):
        return flipped(pz, o, n_pz)

    def copy_z(f, peer, piece=None):
        rows, first = (rows_z, 0) if piece is None else (rows_g, piece * rows_g)
        return pltpu.make_async_remote_copy(
            src_ref=parts_out.at[f, pl.ds(peer * rows_z + first, rows)],
            dst_ref=parts.at[f, pl.ds(pz * rows_z + first, rows)],
            send_sem=send_z.at[f],
            recv_sem=recv_z.at[f if piece is None else f + piece],
            device_id={"pz": peer},
            device_id_type=MESH,
        )

    def wait_for(ref, sem):
        pltpu.make_async_copy(ref, ref, sem).wait()

    def wait_lines(f):
        blocks = n_py - 1 if f else n_py - 2
        wait_for(lines.at[f, pl.ds(0, blocks * rows_y)], recv_y.at[f])
        if f == 0:
            wait_for(lines.at[f, pl.ds(0, rows_y)], recv_y.at[fields])

    mirror = flipped(pz, near, n_pz)
    early = lax.rem(pz, 2) == 0
    pair = lax.rem(pz // 2, 2)

    raw_shares = (tuple(range(0, n_py, 2)), (0, *range(1, n_py, 2)))

    def is_raw(share):
        found = jnp.bool_(False)
        for bit, shares in enumerate(raw_shares):
            for s in shares:
                found = found | ((pair == bit) & (share == s))
        return early & found

    raw_role = is_raw(py)
    plain_role = jnp.logical_not(raw_role)

    def each_pair(do):
        for bit, shares in enumerate(raw_shares):
            pl.when(early & (pair == bit))(functools.partial(do, shares))

    def copy_raw(share):
        return pltpu.make_async_remote_copy(
            src_ref=lines_out.at[0, share],
            dst_ref=far.at[share],
            send_sem=send_raw.at[0],
            recv_sem=recv_raw.at[0],
            device_id={"pz": mirror},
            device_id_type=MESH,
        )

    def send_raws(shares):
        for share in shares:
            copy_raw(share).start()

    def copy_relay(o):
        to = flipped(py, o, n_py)
        return pltpu.make_async_remote_copy(
            src_ref=far.at[to],
            dst_ref=far_lines.at[pl.ds(py * rows_y, rows_y)],
            send_sem=send_relay.at[o],
            recv_sem=recv_relay.at[0],
            device_id={"py": to},
            device_id_type=MESH,
        )

    def copy_far(o):
        to = flipped(pz, o, n_pz)
        return pltpu.make_async_remote_copy(
            src_ref=far_out.at[pl.ds((to - half * near) * rows_z, rows_z)],
            dst_ref=parts.at[0, pl.ds(mirror * rows_z, rows_z)],
            send_sem=send_far.at[0],
            recv_sem=recv_z.at[0],
            device_id={"pz": to},
            device_id_type=MESH,
        )

    last = fields - 1
    late_role = jnp.logical_not(early)

    def send_lines(f, when=None):
        for o in range(1, n_py):
            start = copy_y(f, o).start
            if when is None:
                start()
            else:
                pl.when(is_raw(flipped(py, o, n_py)) == when)(start)

    for f in range(fields):
        load(f).wait()
        high, low = split(held[f])
        if f == 0:
            sides[0].wait()
            for later in range(1, fields):
                load(later).start()
            for side in sides[2:]:
                side.start()
        both = dot(jnp.concatenate([high, low], axis=0), hx[0])
        if f == 0:
            sides[1].wait()
        result = both[:rows_y] + both[rows_y:] + dot(high, hx[1])
        for d in range(n_py):
            lines_out[f, d] = result[:, d * share_x : (d + 1) * share_x]
        if f == 0:
            pl.semaphore_wait(barrier, n_py + n_pz - 2)
            each_pair(send_raws)
            pl.when(late_role)(functools.partial(send_lines, 0))
        elif f < last:
            if f == 1:
                pl.when(early)(functools.partial(send_lines, 0, False))
            pl.when(late_role)(functools.partial(send_lines, f))
        else:
            for held_back in range(1, last):
                pl.when(early)(functools.partial(send_lines, held_back))
            send_lines(0, True)
            send_lines(last)
        lines[f, pl.ds(py * rows_y, rows_y)] = lines_out[f, py]

    for side in sides[2:]:
        side.wait()

    def iota(shape, dim):
        return lax.broadcasted_iota(jnp.int32, shape, dim)

    row, col = iota((depth_y, ny), 0), iota((depth_y, ny), 1)
    pick = (row // zl == col).astype(F32).astype(BF16)
    row, col = iota((ny, depth_y), 0), iota((ny, depth_y), 1)
    spread = (col // zl == row).astype(F32).astype(BF16)
    row, col = iota((depth_y, depth_y), 0), iota((depth_y, depth_y), 1)
    keep = row % zl == col % zl
    for t in range(2):
        wide = dot(dot(pick, hy[t]).astype(BF16), spread)
        my[t] = jnp.where(keep, wide, 0.0).astype(BF16)
    def rows_transform(high_table, low_table, high, low):
        both = dot(high_table, jnp.concatenate([high, low], axis=1))
        return both[:, :share_x] + both[:, share_x:] + dot(low_table, high)

    half_rows = depth_y // 2

    pieces = share_y // group

    def send_parts(f, peers):
        for piece in range(pieces) if f == last else [None]:
            for peer in peers:
                copy_z(f, peer, piece).start()

    deep = lax.rem(pz // (near // 2), 2) == half
    outer = [across(j) for j in range(near // 2)]
    inner = [across(j) for j in range(near // 2, near)]
    around = [beside(o) for o in range(near - 1, 0, -1)]

    def first_quarter(first, rows):
        wait_for(lines.at[0, pl.ds(0, (n_py - 2) * rows_y)], recv_y.at[0])
        span = pl.ds(pl.multiple_of(first, rows), rows)

        def partial(offsets):
            starts = [pl.multiple_of(flipped(py, o, n_py) * rows_y, rows_y) for o in offsets]
            block = jnp.concatenate([lines[0, pl.ds(a, rows_y)] for a in starts], axis=0)
            tables = [
                jnp.concatenate([my[t, span, pl.ds(a, rows_y)] for a in starts], axis=1)
                for t in range(2)
            ]
            return rows_transform(tables[0], tables[1], *split(block))

        near_sum = partial(range(n_py - 1))
        wait_for(lines.at[0, pl.ds(0, rows_y)], recv_y.at[fields])
        parts_out[0, span] = near_sum + partial([n_py - 1])

    def y_step(f, before):
        quarter = half_rows // 2
        far_half = (1 - half) * half_rows
        if f:
            wait_lines(f)
        else:
            first_quarter(far_half + (1 - half) * quarter, quarter)
            send_parts(f, outer)
        high, low = split(lines[f])

        def transform(first, rows):
            span = pl.ds(pl.multiple_of(first, rows), rows)
            parts_out[f, span] = rows_transform(my[0, span], my[1, span], high, low)

        if f:
            transform(far_half + (1 - half) * quarter, quarter)
            send_parts(f, outer)
        transform(far_half + half * quarter, quarter)
        if before is not None:
            pl.when(jnp.logical_not(deep))(functools.partial(send_parts, before, inner))
        if f == last:
            send_parts(f, inner)
        else:
            pl.when(deep)(functools.partial(send_parts, f, inner))
        transform(half * half_rows, half_rows)
        send_parts(f, around)
        parts[f, pl.ds(pz * rows_z, rows_z)] = parts_out[f, pl.ds(pz * rows_z, rows_z)]

    def relay():
        each_pair(lambda shares: wait_for(far.at[pl.ds(0, len(shares))], recv_raw.at[0]))
        for o in range(n_py - 1, 0, -1):
            pl.when(is_raw(flipped(py, o, n_py)))(copy_relay(o).start)

        @pl.when(raw_role)
        def _():
            far_lines[pl.ds(py * rows_y, rows_y)] = far[py]

    def near_step():
        wait_lines(0)
        span = pl.ds(pl.multiple_of(half * half_rows, half_rows), half_rows)
        high, low = split(lines[0])
        parts_out[0, span] = rows_transform(my[0, span], my[1, span], high, low)
        send_parts(0, around)
        parts[0, pl.ds(pz * rows_z, rows_z)] = parts_out[0, pl.ds(pz * rows_z, rows_z)]
        wait_for(far_lines.at[pl.ds(0, (n_py - 1) * rows_y)], recv_relay.at[0])
        high, low = split(far_lines[...])
        far_out[...] = rows_transform(my[0, span], my[1, span], high, low)
        for o in range(near - 1, 0, -1):
            copy_far(o).start()
        parts[0, pl.ds(mirror * rows_z, rows_z)] = far_out[
            pl.ds((pz - half * near) * rows_z, rows_z)
        ]

    pl.when(plain_role)(functools.partial(y_step, 0, None))
    for f in range(1, fields):
        if f == fields - 1:
            pl.when(raw_role)(near_step)
        if f == 1:
            pl.when(plain_role & jnp.logical_not(deep))(functools.partial(send_parts, 0, inner))
        y_step(f, f - 1 if f > 1 else None)
        if f == 1:
            relay()

    row, col = iota((rows_out, nz), 0), iota((rows_out, nz), 1)
    pick = (row % nz == col).astype(F32).astype(BF16)
    row, col = iota((nz, depth_g), 0), iota((nz, depth_g), 1)
    spread = ((col // rows_g) * zl + col % zl == row).astype(F32).astype(BF16)
    row, col = iota((rows_out, depth_g), 0), iota((rows_out, depth_g), 1)
    keep = row // nz == (col // zl) % group
    for t in range(2):
        wide = dot(dot(pick, hz[t]).astype(BF16), spread)
        mz[t] = jnp.where(keep, wide, 0.0).astype(BF16)

    def z_step(f, g):
        starts = [p * rows_z + g * rows_g for p in range(n_pz)]
        block = jnp.concatenate([parts[f, a : a + rows_g] for a in starts], axis=0)
        return rows_transform(mz[0], mz[1], *split(block))

    diagonal = iota((nz, nz), 0) == iota((nz, nz), 1)
    sz_column = jnp.sum(jnp.where(diagonal, sz[...], 0.0), axis=1, keepdims=True)
    sx_row = sx[:, pl.ds(pl.multiple_of(py * share_x, share_x), share_x)]
    for k in range(share_y):
        symbol = (sx_row + sy[pz * share_y + k]) + sz_column
        weights[pl.ds(k * nz, nz)] = 1.0 / (1.0 + symbol)

    def wait_parts(f, blocks):
        wait_for(parts.at[f, pl.ds(0, blocks * rows_z)], recv_z.at[f])

    for f in [*range(1, last), 0, last]:
        if f == 0:
            pl.when(raw_role)(functools.partial(wait_parts, 0, n_pz - 2))
            pl.when(plain_role)(functools.partial(wait_parts, 0, n_pz - 1))
        elif f < last:
            wait_parts(f, n_pz - 1)
        if f < last:
            for g in range(pieces):
                modes[f, pl.ds(g * rows_out, rows_out)] = z_step(f, g)
        if f == 0:
            for k in range(share_y):
                span = pl.ds(k * nz, nz)
                weight = weights[span]
                old = [modes[b, span] for b in range(last)]
                for a in range(fields):
                    mixed = coupling[a, 0] * old[0]
                    for b in range(1, last):
                        mixed = mixed + coupling[a, b] * old[b]
                    mixed = (1.0 - weight) * mixed
                    out_ref[a, span] = mixed + weight * old[a] if a < last else mixed
        if f == last:
            for g in range(pieces):
                wait_for(parts.at[f, pl.ds(0, (n_pz - 1) * rows_g)], recv_z.at[f + g])
                span = pl.ds(g * rows_out, rows_out)
                result = z_step(f, g)
                weight = weights[span]
                rest = (1.0 - weight) * result
                for a in range(fields):
                    new = out_ref[a, span] + coupling[a, last] * rest
                    out_ref[a, span] = new + weight * result if a == last else new
    def sent_parts(f, blocks):
        wait_for(parts_out.at[f, pl.ds(0, blocks * rows_z)], send_z.at[f])

    for f in range(fields):
        wait_for(lines_out.at[f, pl.ds(0, n_py - 1)], send_y.at[f])
        if f:
            sent_parts(f, n_pz - 1)

    each_pair(lambda shares: wait_for(far.at[pl.ds(0, len(shares))], send_raw.at[0]))
    for o in range(1, n_py):
        pl.when(is_raw(flipped(py, o, n_py)))(copy_relay(o).wait_send)

    @pl.when(raw_role)
    def _():
        wait_for(far_out.at[pl.ds(0, (near - 1) * rows_z)], send_far.at[0])
        sent_parts(0, near - 1)

    @pl.when(plain_role)
    def _():
        sent_parts(0, n_pz - 1)


def shards(n_py, n_pz, species, coupling, symbol_x, symbol_y, symbol_z):
    fields, nx, yl, zl = species.shape
    ny, nz = yl * n_py, zl * n_pz
    share_x, share_y = nx // n_py, ny // n_pz
    block = fields * nx * yl * zl
    tables = 2 * (nx * nx + (ny * zl) ** 2 + (share_y * nz) ** 2)
    need = 7 * 4 * block + 2 * tables + 16 * max(ny * zl, share_y * nz) ** 2
    bad = share_x % LANES or zl % SUBLANES or nx % n_py or ny % n_pz
    if bad or need > VMEM_BUDGET or fields < 3 or n_pz % 4 or n_pz & (n_pz - 1):
        return plain_shards(species, coupling, symbol_x, symbol_y, symbol_z)
    dims = (fields, ny, nz, n_py, n_pz, yl, zl, share_x, share_y)
    rows_y, depth_y, depth_z = yl * zl, ny * zl, share_y * nz
    width = nz * max(g for g in range(1, share_y + 1) if share_y % g == 0 and g * nz <= max(nz, 256))
    vmem = pl.BlockSpec(memory_space=pltpu.VMEM)
    hbm = pl.BlockSpec(memory_space=pltpu.HBM)
    values = jnp.transpose(species, (0, 2, 3, 1)).reshape(fields, rows_y, nx)
    out = pl.pallas_call(
        functools.partial(kernel, dims),
        out_shape=jax.ShapeDtypeStruct((fields, depth_z, share_x), F32),
        in_specs=[hbm] * 8,
        out_specs=vmem,
        scratch_shapes=[
            pltpu.VMEM((fields, rows_y, nx), F32),
            pltpu.VMEM((2, nx, nx), BF16),
            pltpu.VMEM((2, ny, ny), BF16),
            pltpu.VMEM((2, nz, nz), BF16),
            pltpu.SMEM((fields, fields), F32),
            pltpu.VMEM((1, nx), F32),
            pltpu.SMEM((ny,), F32),
            pltpu.VMEM((1, nz), F32),
            pltpu.VMEM((fields, n_py, rows_y, share_x), F32),
            pltpu.VMEM((fields, depth_y, share_x), F32),
            pltpu.VMEM((fields, depth_y, share_x), F32),
            pltpu.VMEM((fields, depth_z, share_x), F32),
            pltpu.VMEM((fields - 1, depth_z, share_x), F32),
            pltpu.VMEM((depth_z, share_x), F32),
            pltpu.VMEM((2, depth_y, depth_y), BF16),
            pltpu.VMEM((2, width, width), BF16),
            pltpu.VMEM((n_py, rows_y, share_x), F32),
            pltpu.VMEM((depth_y, share_x), F32),
            pltpu.VMEM((depth_y // 2, share_x), F32),
            pltpu.SemaphoreType.DMA((fields,)),
            pltpu.SemaphoreType.DMA((8,)),
            pltpu.SemaphoreType.DMA((fields,)),
            pltpu.SemaphoreType.DMA((fields + 1,)),
            pltpu.SemaphoreType.DMA((fields,)),
            pltpu.SemaphoreType.DMA((fields + share_y * nz // width - 1,)),
            pltpu.SemaphoreType.DMA((1,)),
            pltpu.SemaphoreType.DMA((1,)),
            pltpu.SemaphoreType.DMA((n_py,)),
            pltpu.SemaphoreType.DMA((1,)),
            pltpu.SemaphoreType.DMA((1,)),
        ],
        compiler_params=pltpu.CompilerParams(
            collective_id=0, has_side_effects=True, vmem_limit_bytes=54500000
        ),
    )(
        *(
            pltpu.with_memory_space_constraint(x, pltpu.HBM)
            for x in (
                values,
                jnp.asarray(split_table(nx)),
                jnp.asarray(split_table(ny)),
                jnp.asarray(split_table(nz)),
                coupling,
                symbol_x.reshape(1, nx),
                symbol_y,
                symbol_z.reshape(1, nz),
            )
        )
    )
    return jnp.transpose(out.reshape(fields, share_y, nz, share_x), (0, 3, 1, 2))


def solution(mesh):
    return jax.shard_map(
        functools.partial(shards, mesh.shape["py"], mesh.shape["pz"]),
        mesh=mesh,
        in_specs=(P(None, None, "py", "pz"), P(), P(), P(), P()),
        out_specs=P(None, "py", "pz", None),
        check_vma=False,
    )
```
